8 devices in a mesh: dp: 2 (over y, z), tp: 4 (over x, core).
Axes of the slice: x: 2, y: 2, z: 1, core: 2. Of those that a mesh axis runs over, the one named last changes fastest.
Arguments:
- x: bfloat16 [2048, 5120], P(('dp', 'tp')), parts along dimension 0
- dy: bfloat16 [2048, 5120], P(('dp', 'tp')), parts along dimension 0
- gain: bfloat16 [5120], replicated
- wq: bfloat16 [5120, 5120], P(None, 'tp')
- wk: bfloat16 [5120, 1024], P(None, 'tp')
- wv: bfloat16 [5120, 1024], P(None, 'tp')
- wo: bfloat16 [5120, 5120], P('tp')
Outputs:
- output 1: bfloat16 [2048, 5120], P(('dp', 'tp')), parts along dimension 0
- output 2: float32 [2, 5120], P('dp'), parts along dimension 0
- output 3: bfloat16 [10240, 5120], P('dp', 'tp'), parts along dimension 0
- output 4: bfloat16 [10240, 1024], P('dp', 'tp'), parts along dimension 0
- output 5: bfloat16 [10240, 1024], P('dp', 'tp'), parts along dimension 0
- output 6: bfloat16 [10240, 5120], P(('dp', 'tp')), parts along dimension 0
There are 2 independent parts. The reference program is written for one: setup_inputs(seed, part) draws one part's arguments, and reference() takes and returns one part's arrays. A program takes and returns all parts, laid end to end along the dimension named above; an argument that names none is the same for every part.
All inputs are finite; a program needn't handle non-finite values.
Results may differ from the reference program's by a relative error of at most 0.018.
Values are sent between devices in bfloat16 or wider.
A program may use at most 2 GiB of HBM per device.

```python
import jax
import jax.numpy as jnp
from jax import lax

ROWS = 1024
D = 5120
HEADS = 40
KV_HEADS = 8
HEAD = 128
THETA = 10000


def setup_inputs(seed: int = 0, part: int = 0) -> dict:
    kx, ky, kn, kq, kk, kv, ko = jax.random.split(jax.random.key(seed), 7)

    def weights(key, rows, columns):
        return jax.random.normal(key, (rows, columns), jnp.float32) * rows**-0.5

    drawn = {
        "x": jax.random.normal(jax.random.fold_in(kx, part), (ROWS, D), jnp.float32),
        "dy": jax.random.normal(jax.random.fold_in(ky, part), (ROWS, D), jnp.float32) * ROWS**-0.5,
        "gain": 1 + 0.1 * jax.random.normal(kn, (D,), jnp.float32),
        "wq": 2 * weights(kq, D, HEADS * HEAD),
        "wk": 2 * weights(kk, D, KV_HEADS * HEAD),
        "wv": 4 * weights(kv, D, KV_HEADS * HEAD),
        "wo": weights(ko, HEADS * HEAD, D),
    }
    return {k: v.astype(jnp.bfloat16) for k, v in drawn.items()}


def normed(x, gain):
    wide = x.astype(jnp.float32)
    scale = lax.rsqrt(jnp.mean(wide * wide, -1, keepdims=True) + 1e-6)
    return (wide * scale * gain.astype(jnp.float32)).astype(jnp.bfloat16)


def turned(t, place, theta):
    half = t.shape[-1] // 2
    angle = place.astype(jnp.float32)[:, None] * theta ** (-jnp.arange(half, dtype=jnp.float32) / half)
    cos, sin = jnp.cos(angle)[:, None], jnp.sin(angle)[:, None]
    a, b = t[..., :half].astype(jnp.float32), t[..., half:].astype(jnp.float32)
    return jnp.concatenate([a * cos - b * sin, b * cos + a * sin], -1).astype(jnp.bfloat16)


def matmul(a, w):
    return jnp.dot(a, w, preferred_element_type=jnp.float32).astype(jnp.bfloat16)


def einsum(form, a, b):
    return jnp.einsum(form, a.astype(jnp.float32), b.astype(jnp.float32))


def attention(q, k, v):
    scores = einsum("tgsd,ugd->gstu", q, k) * q.shape[-1] ** -0.5
    token = jnp.arange(q.shape[0])
    scores = jnp.where(token[:, None] >= token, scores, -jnp.inf)
    weights = jax.nn.softmax(scores, -1).astype(jnp.bfloat16)
    return einsum("gstu,ugd->tgsd", weights, v).astype(jnp.bfloat16)


def forward(x, gain, wq, wk, wv, wo):
    rows = x.shape[0]
    a, place = normed(x, gain), jnp.arange(rows)
    k = turned(matmul(a, wk).reshape(rows, -1, HEAD), place, THETA)
    q = turned(matmul(a, wq).reshape(rows, -1, HEAD), place, THETA).reshape(rows, k.shape[1], -1, HEAD)
    v = matmul(a, wv).reshape(rows, -1, HEAD)
    seen = attention(q, k, v).reshape(rows, -1)
    return (x.astype(jnp.float32) + jnp.dot(seen, wo, preferred_element_type=jnp.float32)).astype(jnp.bfloat16)


def reference(x, dy, gain, wq, wk, wv, wo):
    _, back = jax.vjp(forward, x, gain.astype(jnp.float32), wq, wk, wv, wo)
    by_x, by_gain, *by_weights = back(dy)
    return (by_x, by_gain[None], *by_weights)
```

```python
import functools

import jax
import jax.numpy as jnp
from jax import lax
from jax.experimental import pallas as pl
from jax.experimental.pallas import tpu as pltpu
from jax.sharding import PartitionSpec as P


HEAD = 128
THETA = 10000
LOG2E = 1.4426950408889634
HIDDEN = -2e30
VMEM = 60 * 2**20
OWN = 256
PIECE = 128
QB = 256
TILE = 256
ANY = pl.BlockSpec(memory_space=pl.ANY)


def _dot(a, b, ca, cb):
    return lax.dot_general(a, b, (((ca,), (cb,)), ((), ())), preferred_element_type=jnp.float32)


def _params(n=1):
    return pltpu.CompilerParams(dimension_semantics=("arbitrary",) * n, vmem_limit_bytes=VMEM)


def _cost(flops, nbytes, exps=0):
    return pl.CostEstimate(flops=int(flops), bytes_accessed=int(nbytes), transcendentals=int(exps))


def _project_kernel(pos, x0, x1, gain, c0, c1, s0, s1, wq, wk_any, wv_any, *rest, at, qt, n_alias):
    nx_out, q_out, k_out, v_out, nx_s, wk_s, wv_s, res_s, wsem, nsem, rsem = rest[n_alias:]
    j = pl.program_id(0)

    def nx_copy(p):
        return pltpu.make_async_copy(nx_s.at[pl.ds(p * OWN, OWN)], nx_out.at[pl.ds(pos[at + p] * OWN, OWN)], nsem.at[p])

    def res_copy(p, slot, out, col):
        return pltpu.make_async_copy(res_s.at[slot, pl.ds(p * OWN, OWN)], out.at[pl.ds(pos[at + p] * OWN, OWN), pl.ds(col, TILE)], rsem.at[slot, p])

    wk_copy = pltpu.make_async_copy(wk_any, wk_s, wsem.at[0])
    wv_copy = pltpu.make_async_copy(wv_any, wv_s, wsem.at[1])

    @pl.when(j == 0)
    def _():
        wk_copy.start()
        wv_copy.start()
        for p, ref in enumerate((x0, x1)):
            for r in range(0, OWN, 32):
                wide = ref[r : r + 32].astype(jnp.float32)
                scale = lax.rsqrt(jnp.mean(wide * wide, -1, keepdims=True) + 1e-6)
                nx_s[p * OWN + r : p * OWN + r + 32] = (wide * scale * gain[...].astype(jnp.float32)).astype(jnp.bfloat16)
            nx_copy(p).start()

    def turn(t):
        t = t.astype(jnp.bfloat16).astype(jnp.float32)
        cos = jnp.concatenate([c0[...], c1[...]], 0)
        sin = jnp.concatenate([s0[...], s1[...]], 0)
        heads = [t[:, h : h + HEAD] for h in range(0, TILE, HEAD)]
        return jnp.concatenate([h * cos + pltpu.roll(h, HEAD // 2, 1) * sin for h in heads], 1)

    slot = lax.rem(j, 2)

    @pl.when(j < qt)
    def _():
        @pl.when(j >= 2)
        def _():
            for p in range(2):
                res_copy(p, slot, q_out, pl.multiple_of((j - 2) * TILE, TILE)).wait()

        res_s[slot] = turn(_dot(nx_s[...], wq[...], 1, 0)).astype(jnp.bfloat16)
        for p in range(2):
            res_copy(p, slot, q_out, pl.multiple_of(j * TILE, TILE)).start()

    @pl.when(j == qt)
    def _():
        wk_copy.wait()
        res_s[2] = turn(_dot(nx_s[...], wk_s[...], 1, 0)).astype(jnp.bfloat16)
        for p in range(2):
            res_copy(p, 2, k_out, 0).start()

    @pl.when(j == qt + 1)
    def _():
        wv_copy.wait()
        res_s[3] = _dot(nx_s[...], wv_s[...], 1, 0).astype(jnp.bfloat16)
        for p in range(2):
            res_copy(p, 3, v_out, 0).start()
        for p in range(2):
            nx_copy(p).wait()
            res_copy(p, (qt - 2) % 2, q_out, (qt - 2) * TILE).wait()
            res_copy(p, (qt - 1) % 2, q_out, (qt - 1) * TILE).wait()
            res_copy(p, 2, k_out, 0).wait()
            res_copy(p, 3, v_out, 0).wait()


def project(rows, pos, at, pieces, gain, cos, sin, wq, wk, wv, carry):
    d, nq = wq.shape
    nkv = wk.shape[1]
    qt = nq // TILE
    piece = pl.BlockSpec((OWN, d), lambda j, pos: (0, 0))
    table = lambda p: pl.BlockSpec((OWN, HEAD), lambda j, pos, p=p: (pos[at + p], 0))
    n = 0 if carry is None else 4
    m = 2 * OWN
    return pl.pallas_call(
        functools.partial(_project_kernel, at=at, qt=qt, n_alias=n),
        grid_spec=pltpu.PrefetchScalarGridSpec(
            num_scalar_prefetch=1,
            grid=(qt + 2,),
            in_specs=[piece, piece, pl.BlockSpec((1, d), lambda j, pos: (0, 0)), table(0), table(1), table(0), table(1),
                      pl.BlockSpec((d, TILE), lambda j, pos: (0, jnp.minimum(j, qt - 1))), ANY, ANY] + [ANY] * n,
            out_specs=[ANY] * 4,
            scratch_shapes=[pltpu.VMEM((m, d), jnp.bfloat16), pltpu.VMEM((d, nkv), jnp.bfloat16), pltpu.VMEM((d, nkv), jnp.bfloat16),
                            pltpu.VMEM((4, m, TILE), jnp.bfloat16), pltpu.SemaphoreType.DMA((2,)), pltpu.SemaphoreType.DMA((2,)),
                            pltpu.SemaphoreType.DMA((4, 2))],
        ),
        out_shape=[jax.ShapeDtypeStruct((rows, w), jnp.bfloat16) for w in (d, nq, nkv, nkv)],
        input_output_aliases={11 + i: i for i in range(n)},
        compiler_params=_params(),
        cost_estimate=_cost(2 * m * d * (nq + 2 * nkv), 2 * d * (nq + 2 * nkv)),
        name="project",
    )(pos, *pieces, gain, cos, cos, sin, sin, wq, wk, wv, *(carry or ()))


def _back_out_kernel(pos, *refs, at, size, steps, n, n_alias):
    ys, wo = refs[:n], refs[n]
    dy_out, da_out, y_s, acc_s, res_s, nsem, rsem = refs[n + 1 + n_alias :]
    j = pl.program_id(0)
    step = wo.shape[1]

    def dy_copy(p):
        return pltpu.make_async_copy(y_s.at[pl.ds(p * size, size)], dy_out.at[pl.ds(pos[at + p] * size, size)], nsem.at[p])

    def res_copy(p):
        return pltpu.make_async_copy(res_s.at[:, pl.ds(p * size, size)], da_out.at[:, pl.ds(pl.multiple_of(pos[at + p] * size, size), size)], rsem.at[p])

    @pl.when(j == 0)
    def _():
        for p, ref in enumerate(ys):
            y_s[p * size : (p + 1) * size] = ref[...]
            dy_copy(p).start()

    t = _dot(wo[...], y_s[:, pl.ds(pl.multiple_of(j * step, step), step)], 1, 1)

    @pl.when(j == 0)
    def _():
        acc_s[...] = t

    @pl.when((j > 0) & (j < steps - 1))
    def _():
        acc_s[...] += t

    @pl.when(j == steps - 1)
    def _():
        res_s[...] = (acc_s[...] + t).astype(jnp.bfloat16)
        for p in range(n):
            res_copy(p).start()
        for p in range(n):
            dy_copy(p).wait()
            res_copy(p).wait()


def back_out(rows, pos, at, size, pieces, wo, carry, step=1024):
    nq, d = wo.shape
    n, held = len(pieces), 0 if carry is None else 2
    m = n * size
    return pl.pallas_call(
        functools.partial(_back_out_kernel, at=at, size=size, steps=d // step, n=n, n_alias=held),
        grid_spec=pltpu.PrefetchScalarGridSpec(
            num_scalar_prefetch=1,
            grid=(d // step,),
            in_specs=[pl.BlockSpec((size, d), lambda j, pos: (0, 0))] * n + [pl.BlockSpec((nq, step), lambda j, pos: (0, j))] + [ANY] * held,
            out_specs=[ANY] * 2,
            scratch_shapes=[pltpu.VMEM((m, d), jnp.bfloat16), pltpu.VMEM((nq, m), jnp.float32), pltpu.VMEM((nq, m), jnp.bfloat16),
                            pltpu.SemaphoreType.DMA((n,)), pltpu.SemaphoreType.DMA((n,))],
        ),
        out_shape=[jax.ShapeDtypeStruct((rows, d), jnp.bfloat16), jax.ShapeDtypeStruct((nq, rows), jnp.bfloat16)],
        input_output_aliases={n + 2 + i: i for i in range(held)},
        compiler_params=_params(),
        cost_estimate=_cost(2 * m * d * nq, 2 * d * nq),
        name="back_out",
    )(pos, *pieces, wo, *(carry or ()))


def _forward_kernel(q, k, v, pt, ot, vt_s, *, g, scale):
    rows = q.shape[0]
    e = scale * LOG2E

    @pl.when(lax.rem(pl.program_id(0), g) == 0)
    def _():
        vt_s[...] = v[...].T

    later = lax.broadcasted_iota(jnp.int32, (QB, QB), 0) > lax.broadcasted_iota(jnp.int32, (QB, QB), 1)
    at = 0
    for i in range(rows // QB):
        end = (i + 1) * QB
        s = _dot(k[:end], q[i * QB : end], 1, 1)
        last = jnp.where(later, HIDDEN, s[end - QB :])
        s = last if i == 0 else jnp.concatenate([s[: end - QB], last], 0)
        top = s.max(axis=0, keepdims=True)
        p = jnp.exp2((s - top) * e)
        p = (p * (1 / p.sum(axis=0, keepdims=True))).astype(jnp.bfloat16)
        pt[0, at : at + end] = p
        ot[:, i * QB : end] = _dot(vt_s[:, :end], p, 1, 0).astype(jnp.bfloat16)
        at += end


def attend(q, k, v):
    rows, nq = q.shape
    heads, kv = nq // HEAD, k.shape[1] // HEAD
    g, nb = heads // kv, rows // QB
    kept = QB * nb * (nb + 1) // 2
    column = pl.BlockSpec((rows, HEAD), lambda h: (0, h))
    shared = pl.BlockSpec((rows, HEAD), lambda h: (0, h // g))
    return pl.pallas_call(
        functools.partial(_forward_kernel, g=g, scale=HEAD**-0.5),
        grid=(heads,),
        in_specs=[column, shared, shared],
        out_specs=[pl.BlockSpec((1, kept, QB), lambda h: (h, 0, 0)), pl.BlockSpec((HEAD, rows), lambda h: (h, 0))],
        out_shape=[jax.ShapeDtypeStruct((heads, kept, QB), jnp.bfloat16), jax.ShapeDtypeStruct((nq, rows), jnp.bfloat16)],
        scratch_shapes=[pltpu.VMEM((HEAD, rows), jnp.bfloat16)],
        compiler_params=_params(),
        cost_estimate=_cost(8 * heads * kept * QB * HEAD, 2 * heads * kept * QB, heads * kept * QB),
        name="attend",
    )(q, k, v)


def _backward_kernel(q, k, v, dat, ot, pt, cos, sin, dq, dk, dv, kt_s, dk_s, dv_s, *, g, scale):
    rows = q.shape[0]
    h = lax.rem(pl.program_id(0), g)

    def unturn(t):
        return t * cos[...] - pltpu.roll(t, HEAD // 2, 1) * sin[...]

    @pl.when(h == 0)
    def _():
        kt_s[...] = k[...].T
        dk_s[...] = jnp.zeros_like(dk_s)
        dv_s[...] = jnp.zeros_like(dv_s)

    at = 0
    parts = []
    for i in range(rows // QB):
        end = (i + 1) * QB
        here = slice(i * QB, end)
        p = pt[0, at : at + end]
        wide = p.astype(jnp.float32)
        mine = dat[:, here]
        delta = (mine.astype(jnp.float32) * ot[:, here].astype(jnp.float32)).sum(axis=0, keepdims=True)
        ds = (wide * (_dot(v[:end], mine, 1, 0) - delta)).astype(jnp.bfloat16)
        dv_s[:end] += _dot(p, mine, 1, 1)
        dk_s[:end] += _dot(ds, q[here], 1, 0)
        parts.append(_dot(kt_s[:, :end], ds, 1, 0))
        at += end
    dq[...] = unturn((jnp.concatenate(parts, 1) * scale).T).astype(jnp.bfloat16)

    @pl.when(h == g - 1)
    def _():
        dk[...] = unturn(dk_s[...] * scale).astype(jnp.bfloat16)
        dv[...] = dv_s[...].astype(jnp.bfloat16)


def attend_back(q, k, v, dat, ot, pt, cos, sin):
    rows, nq = q.shape
    heads, kv = nq // HEAD, k.shape[1] // HEAD
    g, kept = heads // kv, pt.shape[1]
    column = pl.BlockSpec((rows, HEAD), lambda h: (0, h))
    shared = pl.BlockSpec((rows, HEAD), lambda h: (0, h // g))
    turned = pl.BlockSpec((HEAD, rows), lambda h: (h, 0))
    table = pl.BlockSpec((rows, HEAD), lambda h: (0, 0))
    return pl.pallas_call(
        functools.partial(_backward_kernel, g=g, scale=HEAD**-0.5),
        grid=(heads,),
        in_specs=[column, shared, shared, turned, turned, pl.BlockSpec((1, kept, QB), lambda h: (h, 0, 0)), table, table],
        out_specs=[column, shared, shared],
        out_shape=[jax.ShapeDtypeStruct(t.shape, jnp.bfloat16) for t in (q, k, v)],
        scratch_shapes=[pltpu.VMEM((HEAD, rows), jnp.bfloat16), pltpu.VMEM((rows, HEAD), jnp.float32), pltpu.VMEM((rows, HEAD), jnp.float32)],
        compiler_params=_params(),
        cost_estimate=_cost(16 * heads * kept * QB * HEAD, 2 * heads * kept * QB),
        name="attend_back",
    )(q, k, v, dat, ot, pt, cos, sin)


def _terms_kernel(pos, *refs, added):
    lhs, w = refs[:6], refs[6:9]
    outs, held = refs[9:-3], refs[-3:]

    @pl.when(pl.program_id(0) == 0)
    def _():
        for p in range(2):
            for i in range(3):
                held[i][p * OWN : (p + 1) * OWN] = lhs[3 * p + i][...]

    t = sum(_dot(held[i][...], w[i][...], 1, 1) for i in range(3))
    if added:
        got, stays, leaves = outs
        t = t + got[...].astype(jnp.float32)
        stays[...] = t[:OWN]
        leaves[...] = t[OWN:].astype(jnp.bfloat16)
    else:
        outs[0][...] = t.astype(jnp.bfloat16)


def terms(pos, at, grads, weights, first, width, got=None, tile=256):
    base = first // tile
    specs = [pl.BlockSpec((OWN, t.shape[1]), lambda j, pos, p=p: (pos[at + p], 0)) for p in range(2) for t in grads]
    specs += [pl.BlockSpec((tile, w.shape[1]), lambda j, pos: (base + j, 0)) for w in weights]
    both = pl.BlockSpec((2 * OWN, tile), lambda j, pos: (0, j))
    one = pl.BlockSpec((OWN, tile), lambda j, pos: (0, j))
    if got is None:
        outs, out_specs, extra = [jax.ShapeDtypeStruct((2 * OWN, width), jnp.bfloat16)], [both], ()
    else:
        outs = [jax.ShapeDtypeStruct((OWN, width), jnp.float32), jax.ShapeDtypeStruct((OWN, width), jnp.bfloat16)]
        out_specs, extra = [one, one], (got,)
        specs.append(both)
    depth = sum(t.shape[1] for t in grads)
    return pl.pallas_call(
        functools.partial(_terms_kernel, added=got is not None),
        grid_spec=pltpu.PrefetchScalarGridSpec(
            num_scalar_prefetch=1, grid=(width // tile,), in_specs=specs, out_specs=out_specs,
            scratch_shapes=[pltpu.VMEM((2 * OWN, t.shape[1]), jnp.bfloat16) for t in grads],
        ),
        out_shape=outs,
        compiler_params=_params(),
        cost_estimate=_cost(4 * OWN * width * depth, 2 * (width * depth + 2 * OWN * depth)),
        name="terms",
    )(pos, *grads, *grads, *weights, *extra)


def _by_qkv_kernel(nx, dq, dk, dv, oq, ok, ov):
    t = nx[...].T
    for g, o in ((dq, oq), (dk, ok), (dv, ov)):
        o[...] = _dot(t, g[...], 1, 0).astype(jnp.bfloat16)


def by_qkv(nx, grads, tile=512):
    rows, d = nx.shape
    whole = [pl.BlockSpec(t.shape, lambda j: (0, 0)) for t in grads]
    depth = sum(t.shape[1] for t in grads)
    return pl.pallas_call(
        _by_qkv_kernel,
        grid=(d // tile,),
        in_specs=[pl.BlockSpec((rows, tile), lambda j: (0, j)), *whole],
        out_specs=[pl.BlockSpec((tile, t.shape[1]), lambda j: (j, 0)) for t in grads],
        out_shape=[jax.ShapeDtypeStruct((d, t.shape[1]), jnp.bfloat16) for t in grads],
        compiler_params=_params(),
        cost_estimate=_cost(2 * rows * d * depth, 2 * d * (rows + depth)),
        name="by_qkv",
    )(nx, *grads)


def _by_out_kernel(ot, dy, o):
    o[...] = _dot(ot[...], dy[...], 1, 0).astype(jnp.bfloat16)


def by_out(ot, dy, tile=512):
    nq, rows = ot.shape
    d = dy.shape[1]
    return pl.pallas_call(
        _by_out_kernel,
        grid=(d // tile,),
        in_specs=[pl.BlockSpec((nq, rows), lambda j: (0, 0)), pl.BlockSpec((rows, tile), lambda j: (0, j))],
        out_specs=pl.BlockSpec((nq, tile), lambda j: (0, j)),
        out_shape=jax.ShapeDtypeStruct((nq, d), jnp.bfloat16),
        compiler_params=_params(),
        cost_estimate=_cost(2 * rows * d * nq, 2 * d * (rows + nq)),
        name="by_out",
    )(ot, dy)


ACROSS = [(0, 2), (1, 3), (2, 0), (3, 1)]
BESIDE = [(0, 1), (1, 0), (2, 3), (3, 2)]
CORNER = [(0, 3), (1, 2), (2, 1), (3, 0)]
CHUNKS = 4


def solution(mesh):
    def step(x, dy, gain, wq, wk, wv, wo):
        me = lax.axis_index("tp")
        own, d = x.shape
        rows = 4 * own
        half = HEAD // 2

        def send(t, way):
            return lax.ppermute(t, "tp", way)

        tie = lax.optimization_barrier

        table = []
        for i in range(4):
            blocks = [i, i ^ 1, (i + 2) % 4, (i + 2) % 4 ^ 1]
            n = own // PIECE
            table.append([blocks[0], blocks[1], blocks[2], blocks[3], blocks[0], blocks[2], blocks[1], blocks[3]]
                         + [n * blocks[b] + p for p in range(n) for b in (2, 3)])
        pos = lax.dynamic_index_in_dim(jnp.array(table, jnp.int32), me, 0, keepdims=False)
        LOCAL, FAR, MINE, THEIRS, FAR_PIECES = 0, 2, 4, 6, 8

        xp = send(x, BESIDE)
        xa = send(x, ACROSS)
        ya = [send(dy[a : a + PIECE], ACROSS) for a in range(0, own, PIECE)]
        yp = send(dy, BESIDE)

        place = jnp.arange(rows)
        angle = place.astype(jnp.float32)[:, None] * THETA ** (-jnp.arange(half, dtype=jnp.float32) / half)
        cos, sin = jnp.cos(angle), jnp.sin(angle)
        cos, sin = jnp.concatenate([cos, cos], 1), jnp.concatenate([-sin, sin], 1)

        row_gain = gain[None]
        near = project(rows, pos, LOCAL, (x, xp), row_gain, cos, sin, wq, wk, wv, None)
        pos_1, near = tie((pos, near))
        back = back_out(rows, pos_1, LOCAL, own, (dy, yp), wo, None)
        xa, near, back = tie((xa, near, back))
        nx, q, k, v = project(rows, pos, FAR, (xa, send(xa, BESIDE)), row_gain, cos, sin, wq, wk, wv, near)
        pt, ot = attend(q, k, v)
        pt, ot, ya, back = tie((pt, ot, ya, back))
        for i, t in enumerate(ya):
            t, back = tie((t, back))
            back = back_out(rows, pos, FAR_PIECES + 2 * i, PIECE, (t, send(t, BESIDE)), wo, back)
        dy_all, dat = back
        grads = attend_back(q, k, v, dat, ot, pt, cos, sin)

        weights = (wq, wk, wv)
        width = d // CHUNKS
        kept, sent, ways = [], [], []
        for c in range(CHUNKS + 1):
            if c < CHUNKS:
                given = terms(pos, THEIRS, grads, weights, c * width, width)[0]
                ways.append(send(given, BESIDE))
            if c > 0:
                got, pos = tie((ways[c - 1], pos)) if c == CHUNKS else tie((ways[c - 1], pos, given))[:2]
                stays, leaves = terms(pos, MINE, grads, weights, (c - 1) * width, width, got)
                stays, leaves, pos = tie((stays, leaves, pos))
                kept.append(stays)
                sent.append(send(leaves, ACROSS))
        nx, dy_all, _ = tie((nx, dy_all, leaves))
        by_weights = by_qkv(nx, grads)
        by_wo = by_out(ot, dy_all)

        g = jnp.concatenate([a + b.astype(jnp.float32) for a, b in zip(kept, sent)], 1)
        wide = x.astype(jnp.float32)
        r = lax.rsqrt(jnp.mean(wide * wide, -1, keepdims=True) + 1e-6)
        unit = wide * r
        by_gain = (g * unit).sum(0, keepdims=True)
        inner = g * gain.astype(jnp.float32)
        by_x = r * (inner - unit * jnp.mean(inner * unit, -1, keepdims=True))
        by_x = (dy.astype(jnp.float32) + by_x).astype(jnp.bfloat16)
        by_gain = by_gain + send(by_gain, BESIDE) + (send(by_gain, ACROSS) + send(by_gain, CORNER))
        return (by_x, by_gain, *by_weights, by_wo)

    tokens, columns = P(("dp", "tp"), None), P(None, "tp")

    return jax.shard_map(
        step,
        mesh=mesh,
        in_specs=(tokens, tokens, P(None), columns, columns, columns, P("tp", None)),
        out_specs=(tokens, P("dp", None), P("dp", "tp"), P("dp", "tp"), P("dp", "tp"), P(("dp", "tp"), None)),
        check_vma=False,
    )
```

```python
import functools

import jax
import jax.numpy as jnp
from jax import lax
from jax.experimental import pallas as pl
from jax.experimental.pallas import tpu as pltpu
from jax.sharding import PartitionSpec as P


HEAD = 128
THETA = 10000
LOG2E = 1.4426950408889634
HIDDEN = -2e30
VMEM = 60 * 2**20
OWN = 256
PIECE = 128
QB = 256
TILE = 256
ANY = pl.BlockSpec(memory_space=pl.ANY)


def _dot(a, b, ca, cb):
    return lax.dot_general(a, b, (((ca,), (cb,)), ((), ())), preferred_element_type=jnp.float32)


def _params(n=1):
    return pltpu.CompilerParams(dimension_semantics=("arbitrary",) * n, vmem_limit_bytes=VMEM)


def _cost(flops, nbytes, exps=0):
    return pl.CostEstimate(flops=int(flops), bytes_accessed=int(nbytes), transcendentals=int(exps))


def _project_kernel(pos, x0, x1, gain, c0, c1, s0, s1, wq, wk_any, wv_any, *rest, at, roles, qt, n_alias):
    nx_out, q_out, k_out, v_out, nx_s, wk_s, wv_s, res_s, wsem, nsem, rsem = rest[n_alias:]
    j = pl.program_id(0)

    def nx_copy(p):
        return pltpu.make_async_copy(nx_s.at[pl.ds(p * OWN, OWN)], nx_out.at[pl.ds(roles[p] * OWN, OWN)], nsem.at[p])

    def res_copy(p, slot, out, col):
        return pltpu.make_async_copy(res_s.at[slot, pl.ds(p * OWN, OWN)], out.at[pl.ds(pos[at + p] * OWN, OWN), pl.ds(col, TILE)], rsem.at[slot, p])

    wk_copy = pltpu.make_async_copy(wk_any, wk_s, wsem.at[0])
    wv_copy = pltpu.make_async_copy(wv_any, wv_s, wsem.at[1])

    @pl.when(j == 0)
    def _():
        wk_copy.start()
        wv_copy.start()
        for p, ref in enumerate((x0, x1)):
            for r in range(0, OWN, 32):
                wide = ref[r : r + 32].astype(jnp.float32)
                scale = lax.rsqrt(jnp.mean(wide * wide, -1, keepdims=True) + 1e-6)
                nx_s[p * OWN + r : p * OWN + r + 32] = (wide * scale * gain[...].astype(jnp.float32)).astype(jnp.bfloat16)
            nx_copy(p).start()

    def turn(t):
        t = t.astype(jnp.bfloat16).astype(jnp.float32)
        cos = jnp.concatenate([c0[...], c1[...]], 0)
        sin = jnp.concatenate([s0[...], s1[...]], 0)
        heads = [t[:, h : h + HEAD] for h in range(0, TILE, HEAD)]
        return jnp.concatenate([h * cos + pltpu.roll(h, HEAD // 2, 1) * sin for h in heads], 1)

    slot = lax.rem(j, 2)

    @pl.when(j < qt)
    def _():
        @pl.when(j >= 2)
        def _():
            for p in range(2):
                res_copy(p, slot, q_out, pl.multiple_of((j - 2) * TILE, TILE)).wait()

        res_s[slot] = turn(_dot(nx_s[...], wq[...], 1, 0)).astype(jnp.bfloat16)
        for p in range(2):
            res_copy(p, slot, q_out, pl.multiple_of(j * TILE, TILE)).start()

    @pl.when(j == qt)
    def _():
        wk_copy.wait()
        res_s[2] = turn(_dot(nx_s[...], wk_s[...], 1, 0)).astype(jnp.bfloat16)
        for p in range(2):
            res_copy(p, 2, k_out, 0).start()

    @pl.when(j == qt + 1)
    def _():
        wv_copy.wait()
        res_s[3] = _dot(nx_s[...], wv_s[...], 1, 0).astype(jnp.bfloat16)
        for p in range(2):
            res_copy(p, 3, v_out, 0).start()
        for p in range(2):
            nx_copy(p).wait()
            res_copy(p, (qt - 2) % 2, q_out, (qt - 2) * TILE).wait()
            res_copy(p, (qt - 1) % 2, q_out, (qt - 1) * TILE).wait()
            res_copy(p, 2, k_out, 0).wait()
            res_copy(p, 3, v_out, 0).wait()


def project(rows, pos, at, roles, pieces, gain, cos, sin, wq, wk, wv, carry):
    d, nq = wq.shape
    nkv = wk.shape[1]
    qt = nq // TILE
    piece = pl.BlockSpec((OWN, d), lambda j, pos: (0, 0))
    table = lambda p: pl.BlockSpec((OWN, HEAD), lambda j, pos, p=p: (pos[at + p], 0))
    n = 0 if carry is None else 4
    m = 2 * OWN
    return pl.pallas_call(
        functools.partial(_project_kernel, at=at, roles=roles, qt=qt, n_alias=n),
        grid_spec=pltpu.PrefetchScalarGridSpec(
            num_scalar_prefetch=1,
            grid=(qt + 2,),
            in_specs=[piece, piece, pl.BlockSpec((1, d), lambda j, pos: (0, 0)), table(0), table(1), table(0), table(1),
                      pl.BlockSpec((d, TILE), lambda j, pos: (0, jnp.minimum(j, qt - 1))), ANY, ANY] + [ANY] * n,
            out_specs=[ANY] * 4,
            scratch_shapes=[pltpu.VMEM((m, d), jnp.bfloat16), pltpu.VMEM((d, nkv), jnp.bfloat16), pltpu.VMEM((d, nkv), jnp.bfloat16),
                            pltpu.VMEM((4, m, TILE), jnp.bfloat16), pltpu.SemaphoreType.DMA((2,)), pltpu.SemaphoreType.DMA((2,)),
                            pltpu.SemaphoreType.DMA((4, 2))],
        ),
        out_shape=[jax.ShapeDtypeStruct((rows, w), jnp.bfloat16) for w in (d, nq, nkv, nkv)],
        input_output_aliases={11 + i: i for i in range(n)},
        compiler_params=_params(),
        cost_estimate=_cost(2 * m * d * (nq + 2 * nkv), 2 * d * (nq + 2 * nkv)),
        name="project",
    )(pos, *pieces, gain, cos, cos, sin, sin, wq, wk, wv, *(carry or ()))


def _back_out_kernel(pos, *refs, at, size, steps, n, n_alias):
    ys, wo = refs[:n], refs[n]
    dy_out, da_out, y_s, acc_s, res_s, nsem, rsem = refs[n + 1 + n_alias :]
    j = pl.program_id(0)
    step = wo.shape[1]

    def dy_copy(p):
        return pltpu.make_async_copy(y_s.at[pl.ds(p * size, size)], dy_out.at[pl.ds(pos[at + p] * size, size)], nsem.at[p])

    def res_copy(p):
        return pltpu.make_async_copy(res_s.at[:, pl.ds(p * size, size)], da_out.at[:, pl.ds(pl.multiple_of(pos[at + p] * size, size), size)], rsem.at[p])

    @pl.when(j == 0)
    def _():
        for p, ref in enumerate(ys):
            y_s[p * size : (p + 1) * size] = ref[...]
            dy_copy(p).start()

    t = _dot(wo[...], y_s[:, pl.ds(pl.multiple_of(j * step, step), step)], 1, 1)

    @pl.when(j == 0)
    def _():
        acc_s[...] = t

    @pl.when((j > 0) & (j < steps - 1))
    def _():
        acc_s[...] += t

    @pl.when(j == steps - 1)
    def _():
        res_s[...] = (acc_s[...] + t).astype(jnp.bfloat16)
        for p in range(n):
            res_copy(p).start()
        for p in range(n):
            dy_copy(p).wait()
            res_copy(p).wait()


def back_out(rows, pos, at, size, pieces, wo, carry, step=1024):
    nq, d = wo.shape
    n, held = len(pieces), 0 if carry is None else 2
    m = n * size
    return pl.pallas_call(
        functools.partial(_back_out_kernel, at=at, size=size, steps=d // step, n=n, n_alias=held),
        grid_spec=pltpu.PrefetchScalarGridSpec(
            num_scalar_prefetch=1,
            grid=(d // step,),
            in_specs=[pl.BlockSpec((size, d), lambda j, pos: (0, 0))] * n + [pl.BlockSpec((nq, step), lambda j, pos: (0, j))] + [ANY] * held,
            out_specs=[ANY] * 2,
            scratch_shapes=[pltpu.VMEM((m, d), jnp.bfloat16), pltpu.VMEM((nq, m), jnp.float32), pltpu.VMEM((nq, m), jnp.bfloat16),
                            pltpu.SemaphoreType.DMA((n,)), pltpu.SemaphoreType.DMA((n,))],
        ),
        out_shape=[jax.ShapeDtypeStruct((rows, d), jnp.bfloat16), jax.ShapeDtypeStruct((nq, rows), jnp.bfloat16)],
        input_output_aliases={n + 2 + i: i for i in range(held)},
        compiler_params=_params(),
        cost_estimate=_cost(2 * m * d * nq, 2 * d * nq),
        name="back_out",
    )(pos, *pieces, wo, *(carry or ()))


def _forward_kernel(q, k, v, pt, ot, vt_s, *, g, scale):
    rows = q.shape[0]
    e = scale * LOG2E

    @pl.when(lax.rem(pl.program_id(0), g) == 0)
    def _():
        vt_s[...] = v[...].T

    later = lax.broadcasted_iota(jnp.int32, (QB, QB), 0) > lax.broadcasted_iota(jnp.int32, (QB, QB), 1)
    at = 0
    for i in range(rows // QB):
        end = (i + 1) * QB
        s = _dot(k[:end], q[i * QB : end], 1, 1)
        last = jnp.where(later, HIDDEN, s[end - QB :])
        s = last if i == 0 else jnp.concatenate([s[: end - QB], last], 0)
        top = s.max(axis=0, keepdims=True)
        p = jnp.exp2((s - top) * e)
        p = (p * (1 / p.sum(axis=0, keepdims=True))).astype(jnp.bfloat16)
        pt[0, at : at + end] = p
        ot[:, i * QB : end] = _dot(vt_s[:, :end], p, 1, 0).astype(jnp.bfloat16)
        at += end


def attend(q, k, v):
    rows, nq = q.shape
    heads, kv = nq // HEAD, k.shape[1] // HEAD
    g, nb = heads // kv, rows // QB
    kept = QB * nb * (nb + 1) // 2
    column = pl.BlockSpec((rows, HEAD), lambda h: (0, h))
    shared = pl.BlockSpec((rows, HEAD), lambda h: (0, h // g))
    return pl.pallas_call(
        functools.partial(_forward_kernel, g=g, scale=HEAD**-0.5),
        grid=(heads,),
        in_specs=[column, shared, shared],
        out_specs=[pl.BlockSpec((1, kept, QB), lambda h: (h, 0, 0)), pl.BlockSpec((HEAD, rows), lambda h: (h, 0))],
        out_shape=[jax.ShapeDtypeStruct((heads, kept, QB), jnp.bfloat16), jax.ShapeDtypeStruct((nq, rows), jnp.bfloat16)],
        scratch_shapes=[pltpu.VMEM((HEAD, rows), jnp.bfloat16)],
        compiler_params=_params(),
        cost_estimate=_cost(8 * heads * kept * QB * HEAD, 2 * heads * kept * QB, heads * kept * QB),
        name="attend",
    )(q, k, v)


def _backward_kernel(pos, q, k, v, dat, ot, pt, cos, sin, dq, dk, dv, kt_s, dk_s, dv_s, *, at_roles, g, scale):
    rows = q.shape[0]
    h = lax.rem(pl.program_id(0), g)

    def unturn(t, here):
        return (t * cos[here] - pltpu.roll(t, HEAD // 2, 1) * sin[here]).astype(jnp.bfloat16)

    def role(i):
        return pl.ds(pl.multiple_of(pos[at_roles + i] * QB, QB), QB)

    @pl.when(h == 0)
    def _():
        kt_s[...] = k[...].T
        dk_s[...] = jnp.zeros_like(dk_s)
        dv_s[...] = jnp.zeros_like(dv_s)

    at = 0
    for i in range(rows // QB):
        end = (i + 1) * QB
        here = slice(i * QB, end)
        p = pt[0, at : at + end]
        mine = dat[:, here]
        delta = (mine.astype(jnp.float32) * ot[:, here].astype(jnp.float32)).sum(axis=0, keepdims=True)
        ds = (p.astype(jnp.float32) * (_dot(v[:end], mine, 1, 0) - delta)).astype(jnp.bfloat16)
        dv_s[:end] += _dot(p, mine, 1, 1)
        dk_s[:end] += _dot(ds, q[here], 1, 0)
        dq[role(i)] = unturn((_dot(kt_s[:, :end], ds, 1, 0) * scale).T, here)
        at += end

    @pl.when(h == g - 1)
    def _():
        for i in range(rows // QB):
            here = slice(i * QB, (i + 1) * QB)
            dk[role(i)] = unturn(dk_s[here] * scale, here)
            dv[role(i)] = dv_s[here].astype(jnp.bfloat16)


def attend_back(pos, at_roles, q, k, v, dat, ot, pt, cos, sin):
    rows, nq = q.shape
    heads, kv = nq // HEAD, k.shape[1] // HEAD
    g, kept = heads // kv, pt.shape[1]
    column = pl.BlockSpec((rows, HEAD), lambda h, pos: (0, h))
    shared = pl.BlockSpec((rows, HEAD), lambda h, pos: (0, h // g))
    turned = pl.BlockSpec((HEAD, rows), lambda h, pos: (h, 0))
    table = pl.BlockSpec((rows, HEAD), lambda h, pos: (0, 0))
    return pl.pallas_call(
        functools.partial(_backward_kernel, at_roles=at_roles, g=g, scale=HEAD**-0.5),
        grid_spec=pltpu.PrefetchScalarGridSpec(
            num_scalar_prefetch=1,
            grid=(heads,),
            in_specs=[column, shared, shared, turned, turned, pl.BlockSpec((1, kept, QB), lambda h, pos: (h, 0, 0)), table, table],
            out_specs=[column, shared, shared],
            scratch_shapes=[pltpu.VMEM((HEAD, rows), jnp.bfloat16), pltpu.VMEM((rows, HEAD), jnp.float32), pltpu.VMEM((rows, HEAD), jnp.float32)],
        ),
        out_shape=[jax.ShapeDtypeStruct(t.shape, jnp.bfloat16) for t in (q, k, v)],
        compiler_params=_params(),
        cost_estimate=_cost(16 * heads * kept * QB * HEAD, 2 * heads * kept * QB),
        name="attend_back",
    )(pos, q, k, v, dat, ot, pt, cos, sin)


def _terms_kernel(q, k, v, a, b, c, stays, leaves, given_s, mine_s, got_s, send_sem, recv_sem):
    j, n = pl.program_id(0), pl.num_programs(0) - 1
    half = 2 * OWN
    me = lax.axis_index("tp")
    partner = {"tp": me + 1 - 2 * lax.rem(me, 2)}

    def hop(i):
        return pltpu.make_async_remote_copy(src_ref=given_s.at[i], dst_ref=got_s.at[i], send_sem=send_sem.at[i], recv_sem=recv_sem.at[i],
                                            device_id=partner, device_id_type=pl.DeviceIdType.MESH)

    @pl.when(j == 0)
    def _():
        barrier = pltpu.get_barrier_semaphore()
        pl.semaphore_signal(barrier, inc=1, device_id=partner, device_id_type=pl.DeviceIdType.MESH)
        pl.semaphore_wait(barrier, 1)

    @pl.when(j < n)
    def _():
        t = sum(_dot(x[...], w[...], 1, 1) for x, w in ((q, a), (k, b), (v, c)))
        given_s[j] = t[:half].astype(jnp.bfloat16)
        mine_s[lax.rem(j, 2)] = t[half:]
        hop(j).start()

    @pl.when(j > 0)
    def _():
        hop(j - 1).wait()
        t = mine_s[lax.rem(j - 1, 2)] + got_s[j - 1].astype(jnp.float32)
        stays[...] = t[:OWN]
        leaves[...] = t[OWN:].astype(jnp.bfloat16)


def terms(number, grads, weights, first, width, tile=512):
    base, n = first // tile, width // tile
    depth = sum(t.shape[1] for t in grads)
    one = pl.BlockSpec((OWN, tile), lambda j: (0, jnp.maximum(j - 1, 0)))
    return pl.pallas_call(
        _terms_kernel,
        grid=(n + 1,),
        in_specs=[pl.BlockSpec(t.shape, lambda j: (0, 0)) for t in grads]
        + [pl.BlockSpec((tile, w.shape[1]), lambda j: (base + jnp.minimum(j, n - 1), 0)) for w in weights],
        out_specs=[one, one],
        out_shape=[jax.ShapeDtypeStruct((OWN, width), jnp.float32), jax.ShapeDtypeStruct((OWN, width), jnp.bfloat16)],
        scratch_shapes=[pltpu.VMEM((n, 2 * OWN, tile), jnp.bfloat16), pltpu.VMEM((2, 2 * OWN, tile), jnp.float32),
                        pltpu.VMEM((n, 2 * OWN, tile), jnp.bfloat16), pltpu.SemaphoreType.DMA((n,)), pltpu.SemaphoreType.DMA((n,))],
        compiler_params=pltpu.CompilerParams(dimension_semantics=("arbitrary",), vmem_limit_bytes=VMEM, collective_id=number, has_side_effects=True),
        cost_estimate=_cost(8 * OWN * width * depth, 2 * width * depth),
        name="terms",
    )(*grads, *weights)


def _finish_kernel(*refs, n):
    stays, came, (x, dy, gain, dx, by_gain) = refs[:n], refs[n : 2 * n], refs[2 * n :]
    wide = x[...].astype(jnp.float32)
    r = lax.rsqrt(jnp.mean(wide * wide, -1, keepdims=True) + 1e-6)
    total, at = 0.0, 0

    @pl.when(pl.program_id(0) == 0)
    def _():
        by_gain[...] = jnp.zeros_like(by_gain)

    for a, b in zip(stays, came):
        here = slice(at, at + a.shape[1])
        g = a[...] + b[...].astype(jnp.float32)
        unit = x[:, here].astype(jnp.float32) * r
        t = g * unit
        by_gain[:, here] += t.sum(0, keepdims=True)
        total = total + (t * gain[:, here].astype(jnp.float32)).sum(-1, keepdims=True)
        at += a.shape[1]
    mean, at = total * (1 / at), 0
    for a, b in zip(stays, came):
        here = slice(at, at + a.shape[1])
        g = a[...] + b[...].astype(jnp.float32)
        unit = x[:, here].astype(jnp.float32) * r
        dx[:, here] = (dy[:, here].astype(jnp.float32) + r * (g * gain[:, here].astype(jnp.float32) - unit * mean)).astype(jnp.bfloat16)
        at += a.shape[1]


def finish(stays, came, x, dy, gain, tile=32):
    own, d = x.shape
    some = lambda t: pl.BlockSpec((tile, t.shape[1]), lambda j: (j, 0))
    whole = pl.BlockSpec((1, d), lambda j: (0, 0))
    return pl.pallas_call(
        functools.partial(_finish_kernel, n=len(stays)),
        grid=(own // tile,),
        in_specs=[some(t) for t in (*stays, *came, x, dy)] + [whole],
        out_specs=[some(x), whole],
        out_shape=[jax.ShapeDtypeStruct((own, d), jnp.bfloat16), jax.ShapeDtypeStruct((1, d), jnp.float32)],
        compiler_params=_params(),
        cost_estimate=_cost(20 * own * d, 14 * own * d),
        name="finish",
    )(*stays, *came, x, dy, gain)


def _by_qkv_kernel(nx, dq, dk, dv, oq, ok, ov):
    t = nx[...].T
    for g, o in ((dq, oq), (dk, ok), (dv, ov)):
        o[...] = _dot(t, g[...], 1, 0).astype(jnp.bfloat16)


def by_qkv(nx, grads, tile=512):
    rows, d = nx.shape
    whole = [pl.BlockSpec(t.shape, lambda j: (0, 0)) for t in grads]
    depth = sum(t.shape[1] for t in grads)
    return pl.pallas_call(
        _by_qkv_kernel,
        grid=(d // tile,),
        in_specs=[pl.BlockSpec((rows, tile), lambda j: (0, j)), *whole],
        out_specs=[pl.BlockSpec((tile, t.shape[1]), lambda j: (j, 0)) for t in grads],
        out_shape=[jax.ShapeDtypeStruct((d, t.shape[1]), jnp.bfloat16) for t in grads],
        compiler_params=_params(),
        cost_estimate=_cost(2 * rows * d * depth, 2 * d * (rows + depth)),
        name="by_qkv",
    )(nx, *grads)


def _by_out_kernel(ot, dy, o):
    o[...] = _dot(ot[...], dy[...], 1, 0).astype(jnp.bfloat16)


def by_out(ot, dy, tile=512):
    nq, rows = ot.shape
    d = dy.shape[1]
    return pl.pallas_call(
        _by_out_kernel,
        grid=(d // tile,),
        in_specs=[pl.BlockSpec((nq, rows), lambda j: (0, 0)), pl.BlockSpec((rows, tile), lambda j: (0, j))],
        out_specs=pl.BlockSpec((nq, tile), lambda j: (0, j)),
        out_shape=jax.ShapeDtypeStruct((nq, d), jnp.bfloat16),
        compiler_params=_params(),
        cost_estimate=_cost(2 * rows * d * nq, 2 * d * (rows + nq)),
        name="by_out",
    )(ot, dy)


ACROSS = [(0, 2), (1, 3), (2, 0), (3, 1)]
BESIDE = [(0, 1), (1, 0), (2, 3), (3, 2)]
CORNER = [(0, 3), (1, 2), (2, 1), (3, 0)]
CHUNKS = (1024, 2048, 2048)


def solution(mesh):
    def step(x, dy, gain, wq, wk, wv, wo):
        me = lax.axis_index("tp")
        own, _ = x.shape
        rows = 4 * own
        half = HEAD // 2

        def send(t, way):
            return lax.ppermute(t, "tp", way)

        tie = lax.optimization_barrier

        table = []
        for i in range(4):
            role = [i ^ 1, (i + 2) % 4 ^ 1, i, (i + 2) % 4]
            n = own // PIECE
            table.append([role[2], role[0], role[3], role[1]] + [n * role[b] + p for p in range(n) for b in (3, 1)] + [role.index(b) for b in range(4)])
        pos = lax.dynamic_index_in_dim(jnp.array(table, jnp.int32), me, 0, keepdims=False)
        LOCAL, FAR, FAR_PIECES = 0, 2, 4
        ROLES = FAR_PIECES + 2 * (own // PIECE)

        xp = send(x, BESIDE)
        xa = send(x, ACROSS)
        ya = [send(dy[a : a + PIECE], ACROSS) for a in range(0, own, PIECE)]
        yp = send(dy, BESIDE)

        place = jnp.arange(rows)
        angle = place.astype(jnp.float32)[:, None] * THETA ** (-jnp.arange(half, dtype=jnp.float32) / half)
        cos, sin = jnp.cos(angle), jnp.sin(angle)
        cos, sin = jnp.concatenate([cos, cos], 1), jnp.concatenate([-sin, sin], 1)

        row_gain = gain[None]
        near = project(rows, pos, LOCAL, (2, 0), (x, xp), row_gain, cos, sin, wq, wk, wv, None)
        pos_1, near = tie((pos, near))
        back = back_out(rows, pos_1, LOCAL, own, (dy, yp), wo, None)
        xa, near, back = tie((xa, near, back))
        nx, q, k, v = project(rows, pos, FAR, (3, 1), (xa, send(xa, BESIDE)), row_gain, cos, sin, wq, wk, wv, near)
        pt, ot = attend(q, k, v)
        pt, ot, ya[0], back = tie((pt, ot, ya[0], back))
        for i, t in enumerate(ya):
            t, back = tie((t, back))
            back = back_out(rows, pos, FAR_PIECES + 2 * i, PIECE, (t, send(t, BESIDE)), wo, back)
        dy_all, dat = back
        grads = attend_back(pos, ROLES, q, k, v, dat, ot, pt, cos, sin)

        weights = (wq, wk, wv)
        first, kept, sent = 0, [], []
        for c, width in enumerate(CHUNKS):
            stays, leaves = terms(c, grads, weights, first, width)
            stays, leaves, grads = tie((stays, leaves, grads))
            kept.append(stays)
            sent.append(send(leaves, ACROSS))
            first += width
        nx, leaves = tie((nx, leaves))
        by_weights = by_qkv(nx, grads)
        dy_all, by_weights = tie((dy_all, by_weights))
        by_wo = by_out(ot, dy_all)
        by_x, by_gain = finish(kept, sent, x, dy, row_gain)
        by_gain = by_gain + send(by_gain, BESIDE) + (send(by_gain, ACROSS) + send(by_gain, CORNER))
        return (by_x, by_gain, *by_weights, by_wo)

    tokens, columns = P(("dp", "tp"), None), P(None, "tp")

    return jax.shard_map(
        step,
        mesh=mesh,
        in_specs=(tokens, tokens, P(None), columns, columns, columns, P("tp", None)),
        out_specs=(tokens, P("dp", None), P("dp", "tp"), P("dp", "tp"), P("dp", "tp"), P(("dp", "tp"), None)),
        check_vma=False,
    )
```

```python
import functools

import jax
import jax.numpy as jnp
from jax import lax
from jax.experimental import pallas as pl
from jax.experimental.pallas import tpu as pltpu
from jax.sharding import PartitionSpec as P


HEAD = 128
THETA = 10000
LOG2E = 1.4426950408889634
HIDDEN = -2e30
VMEM = 60 * 2**20
OWN = 256
PIECE = 128
QB = 256
TILE = 256
ANY = pl.BlockSpec(memory_space=pl.ANY)


def _dot(a, b, ca, cb):
    return lax.dot_general(a, b, (((ca,), (cb,)), ((), ())), preferred_element_type=jnp.float32)


def _params(n=1):
    return pltpu.CompilerParams(dimension_semantics=("arbitrary",) * n, vmem_limit_bytes=VMEM)


def _cost(flops, nbytes, exps=0):
    return pl.CostEstimate(flops=int(flops), bytes_accessed=int(nbytes), transcendentals=int(exps))


def _project_kernel(pos, x0, x1, gain, c0, c1, s0, s1, wq, wk_any, wv_any, *rest, at, roles, qt, n_alias):
    nx_out, q_out, k_out, v_out, nx_s, wk_s, wv_s, res_s, wsem, nsem, rsem = rest[n_alias:]
    j = pl.program_id(0)

    def nx_copy(p):
        return pltpu.make_async_copy(nx_s.at[pl.ds(p * OWN, OWN)], nx_out.at[pl.ds(roles[p] * OWN, OWN)], nsem.at[p])

    def res_copy(p, slot, out, col):
        return pltpu.make_async_copy(res_s.at[slot, pl.ds(p * OWN, OWN)], out.at[pl.ds(pos[at + p] * OWN, OWN), pl.ds(col, TILE)], rsem.at[slot, p])

    wk_copy = pltpu.make_async_copy(wk_any, wk_s, wsem.at[0])
    wv_copy = pltpu.make_async_copy(wv_any, wv_s, wsem.at[1])

    @pl.when(j == 0)
    def _():
        wk_copy.start()
        wv_copy.start()
        for p, ref in enumerate((x0, x1)):
            for r in range(0, OWN, 32):
                wide = ref[r : r + 32].astype(jnp.float32)
                scale = lax.rsqrt(jnp.mean(wide * wide, -1, keepdims=True) + 1e-6)
                nx_s[p * OWN + r : p * OWN + r + 32] = (wide * scale * gain[...].astype(jnp.float32)).astype(jnp.bfloat16)
            nx_copy(p).start()

    def turn(t):
        t = t.astype(jnp.bfloat16).astype(jnp.float32)
        cos = jnp.concatenate([c0[...], c1[...]], 0)
        sin = jnp.concatenate([s0[...], s1[...]], 0)
        heads = [t[:, h : h + HEAD] for h in range(0, TILE, HEAD)]
        return jnp.concatenate([h * cos + pltpu.roll(h, HEAD // 2, 1) * sin for h in heads], 1)

    slot = lax.rem(j, 2)

    @pl.when(j < qt)
    def _():
        @pl.when(j >= 2)
        def _():
            for p in range(2):
                res_copy(p, slot, q_out, pl.multiple_of((j - 2) * TILE, TILE)).wait()

        res_s[slot] = turn(_dot(nx_s[...], wq[...], 1, 0)).astype(jnp.bfloat16)
        for p in range(2):
            res_copy(p, slot, q_out, pl.multiple_of(j * TILE, TILE)).start()

    @pl.when(j == qt)
    def _():
        wk_copy.wait()
        res_s[2] = turn(_dot(nx_s[...], wk_s[...], 1, 0)).astype(jnp.bfloat16)
        for p in range(2):
            res_copy(p, 2, k_out, 0).start()

    @pl.when(j == qt + 1)
    def _():
        wv_copy.wait()
        res_s[3] = _dot(nx_s[...], wv_s[...], 1, 0).astype(jnp.bfloat16)
        for p in range(2):
            res_copy(p, 3, v_out, 0).start()
        for p in range(2):
            nx_copy(p).wait()
            res_copy(p, (qt - 2) % 2, q_out, (qt - 2) * TILE).wait()
            res_copy(p, (qt - 1) % 2, q_out, (qt - 1) * TILE).wait()
            res_copy(p, 2, k_out, 0).wait()
            res_copy(p, 3, v_out, 0).wait()


def project(rows, pos, at, roles, pieces, gain, cos, sin, wq, wk, wv, carry):
    d, nq = wq.shape
    nkv = wk.shape[1]
    qt = nq // TILE
    piece = pl.BlockSpec((OWN, d), lambda j, pos: (0, 0))
    table = lambda p: pl.BlockSpec((OWN, HEAD), lambda j, pos, p=p: (pos[at + p], 0))
    n = 0 if carry is None else 4
    m = 2 * OWN
    return pl.pallas_call(
        functools.partial(_project_kernel, at=at, roles=roles, qt=qt, n_alias=n),
        grid_spec=pltpu.PrefetchScalarGridSpec(
            num_scalar_prefetch=1,
            grid=(qt + 2,),
            in_specs=[piece, piece, pl.BlockSpec((1, d), lambda j, pos: (0, 0)), table(0), table(1), table(0), table(1),
                      pl.BlockSpec((d, TILE), lambda j, pos: (0, jnp.minimum(j, qt - 1))), ANY, ANY] + [ANY] * n,
            out_specs=[ANY] * 4,
            scratch_shapes=[pltpu.VMEM((m, d), jnp.bfloat16), pltpu.VMEM((d, nkv), jnp.bfloat16), pltpu.VMEM((d, nkv), jnp.bfloat16),
                            pltpu.VMEM((4, m, TILE), jnp.bfloat16), pltpu.SemaphoreType.DMA((2,)), pltpu.SemaphoreType.DMA((2,)),
                            pltpu.SemaphoreType.DMA((4, 2))],
        ),
        out_shape=[jax.ShapeDtypeStruct((rows, w), jnp.bfloat16) for w in (d, nq, nkv, nkv)],
        input_output_aliases={11 + i: i for i in range(n)},
        compiler_params=_params(),
        cost_estimate=_cost(2 * m * d * (nq + 2 * nkv), 2 * d * (nq + 2 * nkv)),
        name="project",
    )(pos, *pieces, gain, cos, cos, sin, sin, wq, wk, wv, *(carry or ()))


def _back_out_kernel(pos, *refs, at, size, steps, n, n_alias):
    ys, wo = refs[:n], refs[n]
    dy_out, da_out, y_s, acc_s, res_s, nsem, rsem = refs[n + 1 + n_alias :]
    j = pl.program_id(0)
    step = wo.shape[1]

    def dy_copy(p):
        return pltpu.make_async_copy(y_s.at[pl.ds(p * size, size)], dy_out.at[pl.ds(pos[at + p] * size, size)], nsem.at[p])

    def res_copy(p):
        return pltpu.make_async_copy(res_s.at[:, pl.ds(p * size, size)], da_out.at[:, pl.ds(pl.multiple_of(pos[at + p] * size, size), size)], rsem.at[p])

    @pl.when(j == 0)
    def _():
        for p, ref in enumerate(ys):
            y_s[p * size : (p + 1) * size] = ref[...]
            dy_copy(p).start()

    t = _dot(wo[...], y_s[:, pl.ds(pl.multiple_of(j * step, step), step)], 1, 1)

    @pl.when(j == 0)
    def _():
        acc_s[...] = t

    @pl.when((j > 0) & (j < steps - 1))
    def _():
        acc_s[...] += t

    @pl.when(j == steps - 1)
    def _():
        res_s[...] = (acc_s[...] + t).astype(jnp.bfloat16)
        for p in range(n):
            res_copy(p).start()
        for p in range(n):
            dy_copy(p).wait()
            res_copy(p).wait()


def back_out(rows, pos, at, size, pieces, wo, carry, step=1024):
    nq, d = wo.shape
    n, held = len(pieces), 0 if carry is None else 2
    m = n * size
    return pl.pallas_call(
        functools.partial(_back_out_kernel, at=at, size=size, steps=d // step, n=n, n_alias=held),
        grid_spec=pltpu.PrefetchScalarGridSpec(
            num_scalar_prefetch=1,
            grid=(d // step,),
            in_specs=[pl.BlockSpec((size, d), lambda j, pos: (0, 0))] * n + [pl.BlockSpec((nq, step), lambda j, pos: (0, j))] + [ANY] * held,
            out_specs=[ANY] * 2,
            scratch_shapes=[pltpu.VMEM((m, d), jnp.bfloat16), pltpu.VMEM((nq, m), jnp.float32), pltpu.VMEM((nq, m), jnp.bfloat16),
                            pltpu.SemaphoreType.DMA((n,)), pltpu.SemaphoreType.DMA((n,))],
        ),
        out_shape=[jax.ShapeDtypeStruct((rows, d), jnp.bfloat16), jax.ShapeDtypeStruct((nq, rows), jnp.bfloat16)],
        input_output_aliases={n + 2 + i: i for i in range(held)},
        compiler_params=_params(),
        cost_estimate=_cost(2 * m * d * nq, 2 * d * nq),
        name="back_out",
    )(pos, *pieces, wo, *(carry or ()))


def _forward_kernel(q, k, v, pt, ot, vt_s, *, g, scale):
    rows = q.shape[0]
    e = scale * LOG2E

    @pl.when(lax.rem(pl.program_id(0), g) == 0)
    def _():
        vt_s[...] = v[...].T

    later = lax.broadcasted_iota(jnp.int32, (QB, QB), 0) > lax.broadcasted_iota(jnp.int32, (QB, QB), 1)
    scores = lambda i: _dot(k[: (i + 1) * QB], q[i * QB : (i + 1) * QB], 1, 1)
    ahead, at = scores(0), 0
    for i in range(rows // QB):
        end, s = (i + 1) * QB, ahead
        if end < rows:
            ahead = scores(i + 1)
        last = jnp.where(later, HIDDEN, s[end - QB :])
        s = last if i == 0 else jnp.concatenate([s[: end - QB], last], 0)
        top = s.max(axis=0, keepdims=True)
        p = jnp.exp2((s - top) * e)
        p = (p * (1 / p.sum(axis=0, keepdims=True))).astype(jnp.bfloat16)
        pt[0, at : at + end] = p
        ot[:, i * QB : end] = _dot(vt_s[:, :end], p, 1, 0).astype(jnp.bfloat16)
        at += end


def attend(q, k, v):
    rows, nq = q.shape
    heads, kv = nq // HEAD, k.shape[1] // HEAD
    g, nb = heads // kv, rows // QB
    kept = QB * nb * (nb + 1) // 2
    column = pl.BlockSpec((rows, HEAD), lambda h: (0, h))
    shared = pl.BlockSpec((rows, HEAD), lambda h: (0, h // g))
    return pl.pallas_call(
        functools.partial(_forward_kernel, g=g, scale=HEAD**-0.5),
        grid=(heads,),
        in_specs=[column, shared, shared],
        out_specs=[pl.BlockSpec((1, kept, QB), lambda h: (h, 0, 0)), pl.BlockSpec((HEAD, rows), lambda h: (h, 0))],
        out_shape=[jax.ShapeDtypeStruct((heads, kept, QB), jnp.bfloat16), jax.ShapeDtypeStruct((nq, rows), jnp.bfloat16)],
        scratch_shapes=[pltpu.VMEM((HEAD, rows), jnp.bfloat16)],
        compiler_params=_params(),
        cost_estimate=_cost(8 * heads * kept * QB * HEAD, 2 * heads * kept * QB, heads * kept * QB),
        name="attend",
    )(q, k, v)


def _backward_kernel(pos, q, k, v, dat, ot, pt, cos, sin, dq, dk, dv, kt_s, dk_s, dv_s, *, at_roles, g, scale):
    rows = q.shape[0]
    h = lax.rem(pl.program_id(0), g)

    def unturn(t, here):
        return (t * cos[here] - pltpu.roll(t, HEAD // 2, 1) * sin[here]).astype(jnp.bfloat16)

    def role(i):
        return pl.ds(pl.multiple_of(pos[at_roles + i] * QB, QB), QB)

    @pl.when(h == 0)
    def _():
        kt_s[...] = k[...].T
        dk_s[...] = jnp.zeros_like(dk_s)
        dv_s[...] = jnp.zeros_like(dv_s)

    by_weights = lambda i: _dot(v[: (i + 1) * QB], dat[:, i * QB : (i + 1) * QB], 1, 0)
    ahead, at = by_weights(0), 0
    for i in range(rows // QB):
        end, dp = (i + 1) * QB, ahead
        if end < rows:
            ahead = by_weights(i + 1)
        here = slice(i * QB, end)
        p = pt[0, at : at + end]
        mine = dat[:, here]
        dv_s[:end] += _dot(p, mine, 1, 1)
        delta = (mine.astype(jnp.float32) * ot[:, here].astype(jnp.float32)).sum(axis=0, keepdims=True)
        ds = (p.astype(jnp.float32) * (dp - delta)).astype(jnp.bfloat16)
        dk_s[:end] += _dot(ds, q[here], 1, 0)
        dq[role(i)] = unturn((_dot(kt_s[:, :end], ds, 1, 0) * scale).T, here)
        at += end

    @pl.when(h == g - 1)
    def _():
        for i in range(rows // QB):
            here = slice(i * QB, (i + 1) * QB)
            dk[role(i)] = unturn(dk_s[here] * scale, here)
            dv[role(i)] = dv_s[here].astype(jnp.bfloat16)


def attend_back(pos, at_roles, q, k, v, dat, ot, pt, cos, sin):
    rows, nq = q.shape
    heads, kv = nq // HEAD, k.shape[1] // HEAD
    g, kept = heads // kv, pt.shape[1]
    column = pl.BlockSpec((rows, HEAD), lambda h, pos: (0, h))
    shared = pl.BlockSpec((rows, HEAD), lambda h, pos: (0, h // g))
    turned = pl.BlockSpec((HEAD, rows), lambda h, pos: (h, 0))
    table = pl.BlockSpec((rows, HEAD), lambda h, pos: (0, 0))
    return pl.pallas_call(
        functools.partial(_backward_kernel, at_roles=at_roles, g=g, scale=HEAD**-0.5),
        grid_spec=pltpu.PrefetchScalarGridSpec(
            num_scalar_prefetch=1,
            grid=(heads,),
            in_specs=[column, shared, shared, turned, turned, pl.BlockSpec((1, kept, QB), lambda h, pos: (h, 0, 0)), table, table],
            out_specs=[column, shared, shared],
            scratch_shapes=[pltpu.VMEM((HEAD, rows), jnp.bfloat16), pltpu.VMEM((rows, HEAD), jnp.float32), pltpu.VMEM((rows, HEAD), jnp.float32)],
        ),
        out_shape=[jax.ShapeDtypeStruct(t.shape, jnp.bfloat16) for t in (q, k, v)],
        compiler_params=_params(),
        cost_estimate=_cost(16 * heads * kept * QB * HEAD, 2 * heads * kept * QB),
        name="attend_back",
    )(pos, q, k, v, dat, ot, pt, cos, sin)


def _terms_kernel(q, k, v, a, b, c, stays, leaves, given_s, mine_s, got_s, send_sem, recv_sem):
    j, n = pl.program_id(0), pl.num_programs(0) - 1
    half = 2 * OWN
    me = lax.axis_index("tp")
    partner = {"tp": me + 1 - 2 * lax.rem(me, 2)}

    def hop(i):
        return pltpu.make_async_remote_copy(src_ref=given_s.at[i], dst_ref=got_s.at[i], send_sem=send_sem.at[i], recv_sem=recv_sem.at[i],
                                            device_id=partner, device_id_type=pl.DeviceIdType.MESH)

    @pl.when(j == 0)
    def _():
        barrier = pltpu.get_barrier_semaphore()
        pl.semaphore_signal(barrier, inc=1, device_id=partner, device_id_type=pl.DeviceIdType.MESH)
        pl.semaphore_wait(barrier, 1)

    @pl.when(j < n)
    def _():
        t = sum(_dot(x[...], w[...], 1, 1) for x, w in ((q, a), (k, b), (v, c)))
        given_s[j] = t[:half].astype(jnp.bfloat16)
        mine_s[lax.rem(j, 2)] = t[half:]
        hop(j).start()

    @pl.when(j > 0)
    def _():
        hop(j - 1).wait()
        t = mine_s[lax.rem(j - 1, 2)] + got_s[j - 1].astype(jnp.float32)
        stays[...] = t[:OWN]
        leaves[...] = t[OWN:].astype(jnp.bfloat16)


def terms(number, grads, weights, first, width, tile=512):
    base, n = first // tile, width // tile
    depth = sum(t.shape[1] for t in grads)
    one = pl.BlockSpec((OWN, tile), lambda j: (0, jnp.maximum(j - 1, 0)))
    return pl.pallas_call(
        _terms_kernel,
        grid=(n + 1,),
        in_specs=[pl.BlockSpec(t.shape, lambda j: (0, 0)) for t in grads]
        + [pl.BlockSpec((tile, w.shape[1]), lambda j: (base + jnp.minimum(j, n - 1), 0)) for w in weights],
        out_specs=[one, one],
        out_shape=[jax.ShapeDtypeStruct((OWN, width), jnp.float32), jax.ShapeDtypeStruct((OWN, width), jnp.bfloat16)],
        scratch_shapes=[pltpu.VMEM((n, 2 * OWN, tile), jnp.bfloat16), pltpu.VMEM((2, 2 * OWN, tile), jnp.float32),
                        pltpu.VMEM((n, 2 * OWN, tile), jnp.bfloat16), pltpu.SemaphoreType.DMA((n,)), pltpu.SemaphoreType.DMA((n,))],
        compiler_params=pltpu.CompilerParams(dimension_semantics=("arbitrary",), vmem_limit_bytes=VMEM, collective_id=number, has_side_effects=True),
        cost_estimate=_cost(8 * OWN * width * depth, 2 * width * depth),
        name="terms",
    )(*grads, *weights)


def _finish_kernel(*refs, n):
    stays, came, (x, dy, scale, gain, dx, by_gain) = refs[:n], refs[n : 2 * n], refs[2 * n :]
    r, d = scale[:, :1], x.shape[1]
    step = 512

    @pl.when(pl.program_id(0) == 0)
    def _():
        by_gain[...] = jnp.zeros_like(by_gain)

    def parts():
        at = 0
        for a, b in zip(stays, came):
            for c in range(0, a.shape[1], step):
                yield slice(at + c, at + c + step), a[:, c : c + step] + b[:, c : c + step].astype(jnp.float32)
            at += a.shape[1]

    total = 0.0
    for here, g in parts():
        t = g * (x[:, here].astype(jnp.float32) * r)
        by_gain[:, here] += t.sum(0, keepdims=True)
        total = total + t * gain[:, here]
    mean = total.sum(-1, keepdims=True) * (1 / d)
    cut = mean * r * r
    for here, g in parts():
        t = g * gain[:, here] * r - x[:, here].astype(jnp.float32) * cut
        dx[:, here] = (dy[:, here].astype(jnp.float32) + t).astype(jnp.bfloat16)


def finish(stays, came, x, dy, scale, gain, tile=64):
    own, d = x.shape
    some = lambda t: pl.BlockSpec((tile, t.shape[1]), lambda j: (j, 0))
    whole = pl.BlockSpec((1, d), lambda j: (0, 0))
    return pl.pallas_call(
        functools.partial(_finish_kernel, n=len(stays)),
        grid=(own // tile,),
        in_specs=[some(t) for t in (*stays, *came, x, dy, scale)] + [whole],
        out_specs=[some(x), whole],
        out_shape=[jax.ShapeDtypeStruct((own, d), jnp.bfloat16), jax.ShapeDtypeStruct((1, d), jnp.float32)],
        compiler_params=_params(),
        cost_estimate=_cost(20 * own * d, 14 * own * d),
        name="finish",
    )(*stays, *came, x, dy, scale, gain)


def _by_qkv_kernel(nx, dq, dk, dv, oq, ok, ov):
    t = nx[...].T
    for g, o in ((dq, oq), (dk, ok), (dv, ov)):
        o[...] = _dot(t, g[...], 1, 0).astype(jnp.bfloat16)


def by_qkv(nx, grads, tile=1024):
    rows, d = nx.shape
    whole = [pl.BlockSpec(t.shape, lambda j: (0, 0)) for t in grads]
    depth = sum(t.shape[1] for t in grads)
    return pl.pallas_call(
        _by_qkv_kernel,
        grid=(d // tile,),
        in_specs=[pl.BlockSpec((rows, tile), lambda j: (0, j)), *whole],
        out_specs=[pl.BlockSpec((tile, t.shape[1]), lambda j: (j, 0)) for t in grads],
        out_shape=[jax.ShapeDtypeStruct((d, t.shape[1]), jnp.bfloat16) for t in grads],
        compiler_params=_params(),
        cost_estimate=_cost(2 * rows * d * depth, 2 * d * (rows + depth)),
        name="by_qkv",
    )(nx, *grads)


def _by_out_kernel(ot, dy, o):
    o[...] = _dot(ot[...], dy[...], 1, 0).astype(jnp.bfloat16)


def by_out(ot, dy, tile=1024):
    nq, rows = ot.shape
    d = dy.shape[1]
    return pl.pallas_call(
        _by_out_kernel,
        grid=(d // tile,),
        in_specs=[pl.BlockSpec((nq, rows), lambda j: (0, 0)), pl.BlockSpec((rows, tile), lambda j: (0, j))],
        out_specs=pl.BlockSpec((nq, tile), lambda j: (0, j)),
        out_shape=jax.ShapeDtypeStruct((nq, d), jnp.bfloat16),
        compiler_params=_params(),
        cost_estimate=_cost(2 * rows * d * nq, 2 * d * (rows + nq)),
        name="by_out",
    )(ot, dy)


ACROSS = [(0, 2), (1, 3), (2, 0), (3, 1)]
BESIDE = [(0, 1), (1, 0), (2, 3), (3, 2)]
CORNER = [(0, 3), (1, 2), (2, 1), (3, 0)]
CHUNKS = (2048, 3072)


def solution(mesh):
    def step(x, dy, gain, wq, wk, wv, wo):
        me = lax.axis_index("tp")
        own, _ = x.shape
        rows = 4 * own
        half = HEAD // 2

        def send(t, way):
            return lax.ppermute(t, "tp", way)

        tie = lax.optimization_barrier

        table = []
        for i in range(4):
            role = [i ^ 1, (i + 2) % 4 ^ 1, i, (i + 2) % 4]
            n = own // PIECE
            table.append([role[2], role[0], role[3], role[1]] + [n * role[b] + p for p in range(n) for b in (3, 1)] + [role.index(b) for b in range(4)])
        pos = lax.dynamic_index_in_dim(jnp.array(table, jnp.int32), me, 0, keepdims=False)
        LOCAL, FAR, FAR_PIECES = 0, 2, 4
        ROLES = FAR_PIECES + 2 * (own // PIECE)

        xp = send(x, BESIDE)
        xa = send(x, ACROSS)
        ya = [send(dy[a : a + PIECE], ACROSS) for a in range(0, own, PIECE)]
        yp = send(dy, BESIDE)

        place = jnp.arange(rows)
        angle = place.astype(jnp.float32)[:, None] * THETA ** (-jnp.arange(half, dtype=jnp.float32) / half)
        cos, sin = jnp.cos(angle), jnp.sin(angle)
        cos, sin = jnp.concatenate([cos, cos], 1), jnp.concatenate([-sin, sin], 1)

        row_gain = gain[None]
        near = project(rows, pos, LOCAL, (2, 0), (x, xp), row_gain, cos, sin, wq, wk, wv, None)
        pos_1, near = tie((pos, near))
        back = back_out(rows, pos_1, LOCAL, own, (dy, yp), wo, None)
        xa, near, back = tie((xa, near, back))
        wide, back = tie((x, back))
        wide = wide.astype(jnp.float32)
        scale = jnp.broadcast_to(lax.rsqrt(jnp.mean(wide * wide, -1, keepdims=True) + 1e-6), (own, HEAD))
        nx, q, k, v = project(rows, pos, FAR, (3, 1), (xa, send(xa, BESIDE)), row_gain, cos, sin, wq, wk, wv, near)
        pt, ot = attend(q, k, v)
        pt, ot, ya[0], back = tie((pt, ot, ya[0], back))
        for i, t in enumerate(ya):
            t, back = tie((t, back))
            back = back_out(rows, pos, FAR_PIECES + 2 * i, PIECE, (t, send(t, BESIDE)), wo, back)
        dy_all, dat = back
        grads = attend_back(pos, ROLES, q, k, v, dat, ot, pt, cos, sin)

        weights = (wq, wk, wv)
        first, kept, sent = 0, [], []
        for c, width in enumerate(CHUNKS):
            stays, leaves = terms(c, grads, weights, first, width)
            stays, leaves, grads = tie((stays, leaves, grads))
            kept.append(stays)
            sent.append(send(leaves, ACROSS))
            first += width
        nx, leaves = tie((nx, leaves))
        by_weights = by_qkv(nx, grads)
        dy_all, by_weights = tie((dy_all, by_weights))
        by_wo = by_out(ot, dy_all)
        sent, by_wo = tie((sent, by_wo))
        by_x, by_gain = finish(kept, sent, x, dy, scale, gain.astype(jnp.float32)[None])
        by_gain = by_gain + send(by_gain, BESIDE) + (send(by_gain, ACROSS) + send(by_gain, CORNER))
        return (by_x, by_gain, *by_weights, by_wo)

    tokens, columns = P(("dp", "tp"), None), P(None, "tp")

    return jax.shard_map(
        step,
        mesh=mesh,
        in_specs=(tokens, tokens, P(None), columns, columns, columns, P("tp", None)),
        out_specs=(tokens, P("dp", None), P("dp", "tp"), P("dp", "tp"), P("dp", "tp"), P(("dp", "tp"), None)),
        check_vma=False,
    )
```

```python
import functools

import jax
import jax.numpy as jnp
from jax import lax
from jax.experimental import pallas as pl
from jax.experimental.pallas import tpu as pltpu
from jax.sharding import PartitionSpec as P


HEAD = 128
THETA = 10000
LOG2E = 1.4426950408889634
HIDDEN = -2e30
OWN = 256
PIECE = 128
QB = 256
TILE = 256
BY_TILE = 1024
ANY = pl.BlockSpec(memory_space=pl.ANY)


def _dot(a, b, ca, cb):
    return lax.dot_general(a, b, (((ca,), (cb,)), ((), ())), preferred_element_type=jnp.float32)


def _params(mib, n=1, **rest):
    return pltpu.CompilerParams(dimension_semantics=("arbitrary",) * n, vmem_limit_bytes=mib * 2**20, **rest)


def _cost(flops, nbytes, exps=0):
    return pl.CostEstimate(flops=int(flops), bytes_accessed=int(nbytes), transcendentals=int(exps))


def _project_kernel(pos, x0, x1, gain, c0, c1, s0, s1, wq, wk_any, wv_any, *rest, at, roles, qt, n_alias):
    nx_out, q_out, k_out, v_out, nx_s, wk_s, wv_s, res_s, wsem, nsem, rsem = rest[n_alias:]
    j = pl.program_id(0)

    def nx_copy(p):
        return pltpu.make_async_copy(nx_s.at[pl.ds(p * OWN, OWN)], nx_out.at[pl.ds(roles[p] * OWN, OWN)], nsem.at[p])

    def res_copy(p, slot, out, col):
        return pltpu.make_async_copy(res_s.at[slot, pl.ds(p * OWN, OWN)], out.at[pl.ds(pos[at + p] * OWN, OWN), pl.ds(col, TILE)], rsem.at[slot, p])

    wk_copy = pltpu.make_async_copy(wk_any, wk_s, wsem.at[0])
    wv_copy = pltpu.make_async_copy(wv_any, wv_s, wsem.at[1])

    @pl.when(j == 0)
    def _():
        wk_copy.start()
        wv_copy.start()
        for p, ref in enumerate((x0, x1)):
            for r in range(0, OWN, 32):
                wide = ref[r : r + 32].astype(jnp.float32)
                scale = lax.rsqrt(jnp.mean(wide * wide, -1, keepdims=True) + 1e-6)
                nx_s[p * OWN + r : p * OWN + r + 32] = (wide * scale * gain[...].astype(jnp.float32)).astype(jnp.bfloat16)
            nx_copy(p).start()

    def turn(t):
        t = t.astype(jnp.bfloat16).astype(jnp.float32)
        cos = jnp.concatenate([c0[...], c1[...]], 0)
        sin = jnp.concatenate([s0[...], s1[...]], 0)
        heads = [t[:, h : h + HEAD] for h in range(0, TILE, HEAD)]
        return jnp.concatenate([h * cos + pltpu.roll(h, HEAD // 2, 1) * sin for h in heads], 1)

    slot = lax.rem(j, 2)

    @pl.when(j < qt)
    def _():
        @pl.when(j >= 2)
        def _():
            for p in range(2):
                res_copy(p, slot, q_out, pl.multiple_of((j - 2) * TILE, TILE)).wait()

        res_s[slot] = turn(_dot(nx_s[...], wq[...], 1, 0)).astype(jnp.bfloat16)
        for p in range(2):
            res_copy(p, slot, q_out, pl.multiple_of(j * TILE, TILE)).start()

    @pl.when(j == qt)
    def _():
        wk_copy.wait()
        res_s[2] = turn(_dot(nx_s[...], wk_s[...], 1, 0)).astype(jnp.bfloat16)
        for p in range(2):
            res_copy(p, 2, k_out, 0).start()

    @pl.when(j == qt + 1)
    def _():
        wv_copy.wait()
        res_s[3] = _dot(nx_s[...], wv_s[...], 1, 0).astype(jnp.bfloat16)
        for p in range(2):
            res_copy(p, 3, v_out, 0).start()
        for p in range(2):
            nx_copy(p).wait()
            res_copy(p, (qt - 2) % 2, q_out, (qt - 2) * TILE).wait()
            res_copy(p, (qt - 1) % 2, q_out, (qt - 1) * TILE).wait()
            res_copy(p, 2, k_out, 0).wait()
            res_copy(p, 3, v_out, 0).wait()


def project(rows, pos, at, roles, pieces, gain, cos, sin, wq, wk, wv, carry):
    d, nq = wq.shape
    nkv = wk.shape[1]
    qt = nq // TILE
    piece = pl.BlockSpec((OWN, d), lambda j, pos: (0, 0))
    table = lambda p: pl.BlockSpec((OWN, HEAD), lambda j, pos, p=p: (pos[at + p], 0))
    n = 0 if carry is None else 4
    m = 2 * OWN
    return pl.pallas_call(
        functools.partial(_project_kernel, at=at, roles=roles, qt=qt, n_alias=n),
        grid_spec=pltpu.PrefetchScalarGridSpec(
            num_scalar_prefetch=1,
            grid=(qt + 2,),
            in_specs=[piece, piece, pl.BlockSpec((1, d), lambda j, pos: (0, 0)), table(0), table(1), table(0), table(1),
                      pl.BlockSpec((d, TILE), lambda j, pos: (0, jnp.minimum(j, qt - 1))), ANY, ANY] + [ANY] * n,
            out_specs=[ANY] * 4,
            scratch_shapes=[pltpu.VMEM((m, d), jnp.bfloat16), pltpu.VMEM((d, nkv), jnp.bfloat16), pltpu.VMEM((d, nkv), jnp.bfloat16),
                            pltpu.VMEM((4, m, TILE), jnp.bfloat16), pltpu.SemaphoreType.DMA((2,)), pltpu.SemaphoreType.DMA((2,)),
                            pltpu.SemaphoreType.DMA((4, 2))],
        ),
        out_shape=[jax.ShapeDtypeStruct((rows, w), jnp.bfloat16) for w in (d, nq, nkv, nkv)],
        input_output_aliases={11 + i: i for i in range(n)},
        compiler_params=_params(60),
        cost_estimate=_cost(2 * m * d * (nq + 2 * nkv), 2 * d * (nq + 2 * nkv)),
        name="project",
    )(pos, *pieces, gain, cos, cos, sin, sin, wq, wk, wv, *(carry or ()))


def _back_out_kernel(pos, *refs, at, size, steps, n, n_alias):
    ys, wo = refs[:n], refs[n]
    dy_out, da_out, y_s, acc_s, res_s, nsem, rsem = refs[n + 1 + n_alias :]
    j = pl.program_id(0)
    step = wo.shape[1]

    def dy_copy(p):
        return pltpu.make_async_copy(y_s.at[pl.ds(p * size, size)], dy_out.at[pl.ds(pos[at + p] * size, size)], nsem.at[p])

    def res_copy(p):
        return pltpu.make_async_copy(res_s.at[:, pl.ds(p * size, size)], da_out.at[:, pl.ds(pl.multiple_of(pos[at + p] * size, size), size)], rsem.at[p])

    @pl.when(j == 0)
    def _():
        for p, ref in enumerate(ys):
            y_s[p * size : (p + 1) * size] = ref[...]
            dy_copy(p).start()

    t = _dot(wo[...], y_s[:, pl.ds(pl.multiple_of(j * step, step), step)], 1, 1)

    @pl.when(j == 0)
    def _():
        acc_s[...] = t

    @pl.when((j > 0) & (j < steps - 1))
    def _():
        acc_s[...] += t

    @pl.when(j == steps - 1)
    def _():
        res_s[...] = (acc_s[...] + t).astype(jnp.bfloat16)
        for p in range(n):
            res_copy(p).start()
        for p in range(n):
            dy_copy(p).wait()
            res_copy(p).wait()


def back_out(rows, pos, at, size, pieces, wo, carry, step=1024):
    nq, d = wo.shape
    n, held = len(pieces), 0 if carry is None else 2
    m = n * size
    return pl.pallas_call(
        functools.partial(_back_out_kernel, at=at, size=size, steps=d // step, n=n, n_alias=held),
        grid_spec=pltpu.PrefetchScalarGridSpec(
            num_scalar_prefetch=1,
            grid=(d // step,),
            in_specs=[pl.BlockSpec((size, d), lambda j, pos: (0, 0))] * n + [pl.BlockSpec((nq, step), lambda j, pos: (0, j))] + [ANY] * held,
            out_specs=[ANY] * 2,
            scratch_shapes=[pltpu.VMEM((m, d), jnp.bfloat16), pltpu.VMEM((nq, m), jnp.float32), pltpu.VMEM((nq, m), jnp.bfloat16),
                            pltpu.SemaphoreType.DMA((n,)), pltpu.SemaphoreType.DMA((n,))],
        ),
        out_shape=[jax.ShapeDtypeStruct((rows, d), jnp.bfloat16), jax.ShapeDtypeStruct((nq, rows), jnp.bfloat16)],
        input_output_aliases={n + 2 + i: i for i in range(held)},
        compiler_params=_params(56 if size == OWN else 40),
        cost_estimate=_cost(2 * m * d * nq, 2 * d * nq),
        name="back_out",
    )(pos, *pieces, wo, *(carry or ()))


def _forward_kernel(q, k, v, pt, ot, vt_s, *, g, scale):
    rows = q.shape[0]
    e = scale * LOG2E

    @pl.when(lax.rem(pl.program_id(0), g) == 0)
    def _():
        vt_s[...] = v[...].T

    later = lax.broadcasted_iota(jnp.int32, (QB, QB), 0) > lax.broadcasted_iota(jnp.int32, (QB, QB), 1)
    scores = lambda i: _dot(k[: (i + 1) * QB], q[i * QB : (i + 1) * QB], 1, 1)
    ahead, at = scores(0), 0
    for i in range(rows // QB):
        end, s = (i + 1) * QB, ahead
        if end < rows:
            ahead = scores(i + 1)
        last = jnp.where(later, HIDDEN, s[end - QB :])
        s = last if i == 0 else jnp.concatenate([s[: end - QB], last], 0)
        top = s.max(axis=0, keepdims=True)
        p = jnp.exp2((s - top) * e)
        p = (p * (1 / p.sum(axis=0, keepdims=True))).astype(jnp.bfloat16)
        pt[0, at : at + end] = p
        ot[:, i * QB : end] = _dot(vt_s[:, :end], p, 1, 0).astype(jnp.bfloat16)
        at += end


def attend(q, k, v):
    rows, nq = q.shape
    heads, kv = nq // HEAD, k.shape[1] // HEAD
    g, nb = heads // kv, rows // QB
    kept = QB * nb * (nb + 1) // 2
    column = pl.BlockSpec((rows, HEAD), lambda h: (0, h))
    shared = pl.BlockSpec((rows, HEAD), lambda h: (0, h // g))
    return pl.pallas_call(
        functools.partial(_forward_kernel, g=g, scale=HEAD**-0.5),
        grid=(heads,),
        in_specs=[column, shared, shared],
        out_specs=[pl.BlockSpec((1, kept, QB), lambda h: (h, 0, 0)), pl.BlockSpec((HEAD, rows), lambda h: (h, 0))],
        out_shape=[jax.ShapeDtypeStruct((heads, kept, QB), jnp.bfloat16), jax.ShapeDtypeStruct((nq, rows), jnp.bfloat16)],
        scratch_shapes=[pltpu.VMEM((HEAD, rows), jnp.bfloat16)],
        compiler_params=_params(58),
        cost_estimate=_cost(8 * heads * kept * QB * HEAD, 2 * heads * kept * QB, heads * kept * QB),
        name="attend",
    )(q, k, v)


def _backward_kernel(pos, q, k, v, dat, ot, pt, cos, sin, dq, dk, dv, kt_s, dk_s, dv_s, *, at_roles, g, scale):
    rows = q.shape[0]
    h = lax.rem(pl.program_id(0), g)

    def unturn(t, here):
        return (t * cos[here] - pltpu.roll(t, HEAD // 2, 1) * sin[here]).astype(jnp.bfloat16)

    def role(i):
        return pl.ds(pl.multiple_of(pos[at_roles + i] * QB, QB), QB)

    @pl.when(h == 0)
    def _():
        kt_s[...] = k[...].T
        dk_s[...] = jnp.zeros_like(dk_s)
        dv_s[...] = jnp.zeros_like(dv_s)

    by_weights = lambda i: _dot(v[: (i + 1) * QB], dat[:, i * QB : (i + 1) * QB], 1, 0)
    ahead, at = by_weights(0), 0
    for i in range(rows // QB):
        end, dp = (i + 1) * QB, ahead
        if end < rows:
            ahead = by_weights(i + 1)
        here = slice(i * QB, end)
        p = pt[0, at : at + end]
        mine = dat[:, here]
        dv_s[:end] += _dot(p, mine, 1, 1)
        delta = (mine.astype(jnp.float32) * ot[:, here].astype(jnp.float32)).sum(axis=0, keepdims=True)
        ds = (p.astype(jnp.float32) * (dp - delta)).astype(jnp.bfloat16)
        dk_s[:end] += _dot(ds, q[here], 1, 0)
        dq[role(i)] = unturn((_dot(kt_s[:, :end], ds, 1, 0) * scale).T, here)
        at += end

    @pl.when(h == g - 1)
    def _():
        for i in range(rows // QB):
            here = slice(i * QB, (i + 1) * QB)
            dk[role(i)] = unturn(dk_s[here] * scale, here)
            dv[role(i)] = dv_s[here].astype(jnp.bfloat16)


def attend_back(pos, at_roles, q, k, v, dat, ot, pt, cos, sin):
    rows, nq = q.shape
    heads, kv = nq // HEAD, k.shape[1] // HEAD
    g, kept = heads // kv, pt.shape[1]
    column = pl.BlockSpec((rows, HEAD), lambda h, pos: (0, h))
    shared = pl.BlockSpec((rows, HEAD), lambda h, pos: (0, h // g))
    turned = pl.BlockSpec((HEAD, rows), lambda h, pos: (h, 0))
    table = pl.BlockSpec((rows, HEAD), lambda h, pos: (0, 0))
    return pl.pallas_call(
        functools.partial(_backward_kernel, at_roles=at_roles, g=g, scale=HEAD**-0.5),
        grid_spec=pltpu.PrefetchScalarGridSpec(
            num_scalar_prefetch=1,
            grid=(heads,),
            in_specs=[column, shared, shared, turned, turned, pl.BlockSpec((1, kept, QB), lambda h, pos: (h, 0, 0)), table, table],
            out_specs=[column, shared, shared],
            scratch_shapes=[pltpu.VMEM((HEAD, rows), jnp.bfloat16), pltpu.VMEM((rows, HEAD), jnp.float32), pltpu.VMEM((rows, HEAD), jnp.float32)],
        ),
        out_shape=[jax.ShapeDtypeStruct(t.shape, jnp.bfloat16) for t in (q, k, v)],
        compiler_params=_params(36),
        cost_estimate=_cost(16 * heads * kept * QB * HEAD, 2 * heads * kept * QB),
        name="attend_back",
    )(pos, q, k, v, dat, ot, pt, cos, sin)


def _terms_kernel(q, k, v, a, b, c, stays, leaves, given_s, mine_s, got_s, send_sem, recv_sem):
    j, n = pl.program_id(0), pl.num_programs(0) - 1
    half = 2 * OWN
    me = lax.axis_index("tp")
    partner = {"tp": me + 1 - 2 * lax.rem(me, 2)}

    def hop(i):
        return pltpu.make_async_remote_copy(src_ref=given_s.at[i], dst_ref=got_s.at[i], send_sem=send_sem.at[i], recv_sem=recv_sem.at[i],
                                            device_id=partner, device_id_type=pl.DeviceIdType.MESH)

    @pl.when(j == 0)
    def _():
        barrier = pltpu.get_barrier_semaphore()
        pl.semaphore_signal(barrier, inc=1, device_id=partner, device_id_type=pl.DeviceIdType.MESH)
        pl.semaphore_wait(barrier, 1)

    @pl.when(j < n)
    def _():
        some = lambda rows: sum(_dot(x[rows], w[...], 1, 1) for x, w in ((q, a), (k, b), (v, c)))
        given_s[j] = some(slice(0, half)).astype(jnp.bfloat16)
        hop(j).start()
        mine_s[lax.rem(j, 2)] = some(slice(half, 2 * half))

    @pl.when(j > 0)
    def _():
        hop(j - 1).wait()
        t = mine_s[lax.rem(j - 1, 2)] + got_s[j - 1].astype(jnp.float32)
        stays[...] = t[:OWN]
        leaves[...] = t[OWN:].astype(jnp.bfloat16)


def terms(number, grads, weights, first, width, tile=512):
    base, n = first // tile, width // tile
    depth = sum(t.shape[1] for t in grads)
    one = pl.BlockSpec((OWN, tile), lambda j: (0, jnp.maximum(j - 1, 0)))
    return pl.pallas_call(
        _terms_kernel,
        grid=(n + 1,),
        in_specs=[pl.BlockSpec(t.shape, lambda j: (0, 0)) for t in grads]
        + [pl.BlockSpec((tile, w.shape[1]), lambda j: (base + jnp.minimum(j, n - 1), 0)) for w in weights],
        out_specs=[one, one],
        out_shape=[jax.ShapeDtypeStruct((OWN, width), jnp.float32), jax.ShapeDtypeStruct((OWN, width), jnp.bfloat16)],
        scratch_shapes=[pltpu.VMEM((n, 2 * OWN, tile), jnp.bfloat16), pltpu.VMEM((2, 2 * OWN, tile), jnp.float32),
                        pltpu.VMEM((n, 2 * OWN, tile), jnp.bfloat16), pltpu.SemaphoreType.DMA((n,)), pltpu.SemaphoreType.DMA((n,))],
        compiler_params=_params(54, collective_id=number, has_side_effects=True),
        cost_estimate=_cost(8 * OWN * width * depth, 2 * width * depth),
        name="terms",
    )(*grads, *weights)


def _finish_kernel(*refs, n):
    stays, came, (x, dy, scale, gain, dx, by_gain) = refs[:n], refs[n : 2 * n], refs[2 * n :]
    r, d = scale[:, :1], x.shape[1]
    step = 512

    @pl.when(pl.program_id(0) == 0)
    def _():
        by_gain[...] = jnp.zeros_like(by_gain)

    def parts():
        at = 0
        for a, b in zip(stays, came):
            for c in range(0, a.shape[1], step):
                yield slice(at + c, at + c + step), a[:, c : c + step] + b[:, c : c + step].astype(jnp.float32)
            at += a.shape[1]

    total = 0.0
    for here, g in parts():
        t = g * (x[:, here].astype(jnp.float32) * r)
        by_gain[:, here] += t.sum(0, keepdims=True)
        total = total + t * gain[:, here]
    mean = total.sum(-1, keepdims=True) * (1 / d)
    cut = mean * r * r
    for here, g in parts():
        t = g * gain[:, here] * r - x[:, here].astype(jnp.float32) * cut
        dx[:, here] = (dy[:, here].astype(jnp.float32) + t).astype(jnp.bfloat16)


def finish(stays, came, x, dy, scale, gain, tile=64):
    own, d = x.shape
    some = lambda t: pl.BlockSpec((tile, t.shape[1]), lambda j: (j, 0))
    whole = pl.BlockSpec((1, d), lambda j: (0, 0))
    return pl.pallas_call(
        functools.partial(_finish_kernel, n=len(stays)),
        grid=(own // tile,),
        in_specs=[some(t) for t in (*stays, *came, x, dy, scale)] + [whole],
        out_specs=[some(x), whole],
        out_shape=[jax.ShapeDtypeStruct((own, d), jnp.bfloat16), jax.ShapeDtypeStruct((1, d), jnp.float32)],
        compiler_params=_params(14),
        cost_estimate=_cost(20 * own * d, 14 * own * d),
        name="finish",
    )(*stays, *came, x, dy, scale, gain)


def _by_weights_kernel(nx, dq, dk, dv, ot, dy, oq, ok, ov, oo):
    t = nx[...].T
    for g, o in ((dq, oq), (dk, ok), (dv, ov)):
        o[...] = _dot(t, g[...], 1, 0).astype(jnp.bfloat16)
    oo[...] = _dot(ot[...], dy[...], 1, 0).astype(jnp.bfloat16)


def by_weights(nx, grads, ot, dy, tile=BY_TILE):
    rows, d = nx.shape
    nq = ot.shape[0]
    whole = lambda t: pl.BlockSpec(t.shape, lambda j: (0, 0))
    columns = lambda n: pl.BlockSpec((n, tile), lambda j: (0, j))
    depth = sum(t.shape[1] for t in grads)
    return pl.pallas_call(
        _by_weights_kernel,
        grid=(d // tile,),
        in_specs=[columns(rows), *map(whole, grads), whole(ot), columns(rows)],
        out_specs=[pl.BlockSpec((tile, t.shape[1]), lambda j: (j, 0)) for t in grads] + [columns(nq)],
        out_shape=[jax.ShapeDtypeStruct((d, t.shape[1]), jnp.bfloat16) for t in grads] + [jax.ShapeDtypeStruct((nq, d), jnp.bfloat16)],
        compiler_params=_params(40),
        cost_estimate=_cost(2 * rows * d * (depth + nq), 2 * d * (2 * rows + depth + nq)),
        name="by_weights",
    )(nx, *grads, ot, dy)


ACROSS = [(0, 2), (1, 3), (2, 0), (3, 1)]
BESIDE = [(0, 1), (1, 0), (2, 3), (3, 2)]
CORNER = [(0, 3), (1, 2), (2, 1), (3, 0)]
CHUNKS = (2048, 3072)


def solution(mesh):
    def step(x, dy, gain, wq, wk, wv, wo):
        me = lax.axis_index("tp")
        own, _ = x.shape
        rows = 4 * own
        half = HEAD // 2

        def send(t, way):
            return lax.ppermute(t, "tp", way)

        tie = lax.optimization_barrier

        table = []
        for i in range(4):
            role = [i ^ 1, (i + 2) % 4 ^ 1, i, (i + 2) % 4]
            n = own // PIECE
            table.append([role[2], role[0], role[3], role[1]] + [n * role[b] + p for p in range(n) for b in (3, 1)] + [role.index(b) for b in range(4)])
        pos = lax.dynamic_index_in_dim(jnp.array(table, jnp.int32), me, 0, keepdims=False)
        LOCAL, FAR, FAR_PIECES = 0, 2, 4
        ROLES = FAR_PIECES + 2 * (own // PIECE)

        xp = send(x, BESIDE)
        xa = send(x, ACROSS)
        ya = [send(dy[a : a + PIECE], ACROSS) for a in range(0, own, PIECE)]
        yp = send(dy, BESIDE)

        place = jnp.arange(rows)
        angle = place.astype(jnp.float32)[:, None] * THETA ** (-jnp.arange(half, dtype=jnp.float32) / half)
        cos, sin = jnp.cos(angle), jnp.sin(angle)
        cos, sin = jnp.concatenate([cos, cos], 1), jnp.concatenate([-sin, sin], 1)

        row_gain = gain[None]
        near = project(rows, pos, LOCAL, (2, 0), (x, xp), row_gain, cos, sin, wq, wk, wv, None)
        pos_1, near = tie((pos, near))
        back = back_out(rows, pos_1, LOCAL, own, (dy, yp), wo, None)
        xa, near, back = tie((xa, near, back))
        wide, back = tie((x, back))
        wide = wide.astype(jnp.float32)
        scale = jnp.broadcast_to(lax.rsqrt(jnp.mean(wide * wide, -1, keepdims=True) + 1e-6), (own, HEAD))
        nx, q, k, v = project(rows, pos, FAR, (3, 1), (xa, send(xa, BESIDE)), row_gain, cos, sin, wq, wk, wv, near)
        pt, ot = attend(q, k, v)
        pt, ot, ya[0], back = tie((pt, ot, ya[0], back))
        for i, t in enumerate(ya):
            t, back = tie((t, back))
            back = back_out(rows, pos, FAR_PIECES + 2 * i, PIECE, (t, send(t, BESIDE)), wo, back)
        dy_all, dat = back
        grads = attend_back(pos, ROLES, q, k, v, dat, ot, pt, cos, sin)

        weights = (wq, wk, wv)
        first, kept, sent = 0, [], []
        for c, width in enumerate(CHUNKS):
            stays, leaves = terms(c, grads, weights, first, width)
            stays, leaves, grads = tie((stays, leaves, grads))
            kept.append(stays)
            sent.append(send(leaves, ACROSS))
            first += width
        nx, leaves = tie((nx, leaves))
        *by_qkv, by_wo = by_weights(nx, grads, ot, dy_all)
        sent, by_wo = tie((sent, by_wo))
        by_x, by_gain = finish(kept, sent, x, dy, scale, gain.astype(jnp.float32)[None])
        by_gain = by_gain + send(by_gain, BESIDE) + (send(by_gain, ACROSS) + send(by_gain, CORNER))
        return (by_x, by_gain, *by_qkv, by_wo)

    tokens, columns = P(("dp", "tp"), None), P(None, "tp")

    return jax.shard_map(
        step,
        mesh=mesh,
        in_specs=(tokens, tokens, P(None), columns, columns, columns, P("tp", None)),
        out_specs=(tokens, P("dp", None), P("dp", "tp"), P("dp", "tp"), P("dp", "tp"), P(("dp", "tp"), None)),
        check_vma=False,
    )
```

```python
import functools

import jax
import jax.numpy as jnp
from jax import lax
from jax.experimental import pallas as pl
from jax.experimental.pallas import tpu as pltpu
from jax.sharding import PartitionSpec as P


HEAD = 128
THETA = 10000
LOG2E = 1.4426950408889634
HIDDEN = -2e30
OWN = 256
PIECE = 128
QB = 256
TILE = 256
BY_TILE = 512
ANY = pl.BlockSpec(memory_space=pl.ANY)


def _dot(a, b, ca, cb):
    return lax.dot_general(a, b, (((ca,), (cb,)), ((), ())), preferred_element_type=jnp.float32)


def _params(mib, n=1, **rest):
    return pltpu.CompilerParams(dimension_semantics=("arbitrary",) * n, vmem_limit_bytes=mib * 2**20, **rest)


def _cost(flops, nbytes, exps=0):
    return pl.CostEstimate(flops=int(flops), bytes_accessed=int(nbytes), transcendentals=int(exps))


def _project_kernel(pos, x0, x1, gain, c0, c1, s0, s1, wq, wk_any, wv_any, *rest, at, roles, qt, n_alias):
    nx_out, q_out, k_out, v_out, nx_s, wk_s, wv_s, res_s, wsem, nsem, rsem = rest[n_alias:]
    j = pl.program_id(0)

    def nx_copy(p):
        return pltpu.make_async_copy(nx_s.at[pl.ds(p * OWN, OWN)], nx_out.at[pl.ds(roles[p] * OWN, OWN)], nsem.at[p])

    def res_copy(p, slot, out, col):
        return pltpu.make_async_copy(res_s.at[slot, pl.ds(p * OWN, OWN)], out.at[pl.ds(pos[at + p] * OWN, OWN), pl.ds(col, TILE)], rsem.at[slot, p])

    wk_copy = pltpu.make_async_copy(wk_any, wk_s, wsem.at[0])
    wv_copy = pltpu.make_async_copy(wv_any, wv_s, wsem.at[1])

    @pl.when(j == 0)
    def _():
        wk_copy.start()
        wv_copy.start()
        for p, ref in enumerate((x0, x1)):
            for r in range(0, OWN, 32):
                wide = ref[r : r + 32].astype(jnp.float32)
                scale = lax.rsqrt(jnp.mean(wide * wide, -1, keepdims=True) + 1e-6)
                nx_s[p * OWN + r : p * OWN + r + 32] = (wide * scale * gain[...].astype(jnp.float32)).astype(jnp.bfloat16)
            nx_copy(p).start()

    def turn(t):
        t = t.astype(jnp.bfloat16).astype(jnp.float32)
        cos = jnp.concatenate([c0[...], c1[...]], 0)
        sin = jnp.concatenate([s0[...], s1[...]], 0)
        heads = [t[:, h : h + HEAD] for h in range(0, TILE, HEAD)]
        return jnp.concatenate([h * cos + pltpu.roll(h, HEAD // 2, 1) * sin for h in heads], 1)

    slot = lax.rem(j, 2)

    @pl.when(j < qt)
    def _():
        @pl.when(j >= 2)
        def _():
            for p in range(2):
                res_copy(p, slot, q_out, pl.multiple_of((j - 2) * TILE, TILE)).wait()

        res_s[slot] = turn(_dot(nx_s[...], wq[...], 1, 0)).astype(jnp.bfloat16)
        for p in range(2):
            res_copy(p, slot, q_out, pl.multiple_of(j * TILE, TILE)).start()

    @pl.when(j == qt)
    def _():
        wk_copy.wait()
        res_s[2] = turn(_dot(nx_s[...], wk_s[...], 1, 0)).astype(jnp.bfloat16)
        for p in range(2):
            res_copy(p, 2, k_out, 0).start()

    @pl.when(j == qt + 1)
    def _():
        wv_copy.wait()
        res_s[3] = _dot(nx_s[...], wv_s[...], 1, 0).astype(jnp.bfloat16)
        for p in range(2):
            res_copy(p, 3, v_out, 0).start()
        for p in range(2):
            nx_copy(p).wait()
            res_copy(p, (qt - 2) % 2, q_out, (qt - 2) * TILE).wait()
            res_copy(p, (qt - 1) % 2, q_out, (qt - 1) * TILE).wait()
            res_copy(p, 2, k_out, 0).wait()
            res_copy(p, 3, v_out, 0).wait()


def project(rows, pos, at, roles, pieces, gain, cos, sin, wq, wk, wv, carry):
    d, nq = wq.shape
    nkv = wk.shape[1]
    qt = nq // TILE
    piece = pl.BlockSpec((OWN, d), lambda j, pos: (0, 0))
    table = lambda p: pl.BlockSpec((OWN, HEAD), lambda j, pos, p=p: (pos[at + p], 0))
    n = 0 if carry is None else 4
    m = 2 * OWN
    return pl.pallas_call(
        functools.partial(_project_kernel, at=at, roles=roles, qt=qt, n_alias=n),
        grid_spec=pltpu.PrefetchScalarGridSpec(
            num_scalar_prefetch=1,
            grid=(qt + 2,),
            in_specs=[piece, piece, pl.BlockSpec((1, d), lambda j, pos: (0, 0)), table(0), table(1), table(0), table(1),
                      pl.BlockSpec((d, TILE), lambda j, pos: (0, jnp.minimum(j, qt - 1))), ANY, ANY] + [ANY] * n,
            out_specs=[ANY] * 4,
            scratch_shapes=[pltpu.VMEM((m, d), jnp.bfloat16), pltpu.VMEM((d, nkv), jnp.bfloat16), pltpu.VMEM((d, nkv), jnp.bfloat16),
                            pltpu.VMEM((4, m, TILE), jnp.bfloat16), pltpu.SemaphoreType.DMA((2,)), pltpu.SemaphoreType.DMA((2,)),
                            pltpu.SemaphoreType.DMA((4, 2))],
        ),
        out_shape=[jax.ShapeDtypeStruct((rows, w), jnp.bfloat16) for w in (d, nq, nkv, nkv)],
        input_output_aliases={11 + i: i for i in range(n)},
        compiler_params=_params(60),
        cost_estimate=_cost(2 * m * d * (nq + 2 * nkv), 2 * d * (nq + 2 * nkv)),
        name="project",
    )(pos, *pieces, gain, cos, cos, sin, sin, wq, wk, wv, *(carry or ()))


def _back_out_kernel(pos, *refs, at, size, steps, n, n_alias):
    ys, wo = refs[:n], refs[n]
    dy_out, da_out, y_s, acc_s, res_s, nsem, rsem = refs[n + 1 + n_alias :]
    j = pl.program_id(0)
    step = wo.shape[1]

    def dy_copy(p):
        return pltpu.make_async_copy(y_s.at[pl.ds(p * size, size)], dy_out.at[pl.ds(pos[at + p] * size, size)], nsem.at[p])

    def res_copy(p):
        return pltpu.make_async_copy(res_s.at[:, pl.ds(p * size, size)], da_out.at[:, pl.ds(pl.multiple_of(pos[at + p] * size, size), size)], rsem.at[p])

    @pl.when(j == 0)
    def _():
        for p, ref in enumerate(ys):
            y_s[p * size : (p + 1) * size] = ref[...]
            dy_copy(p).start()

    t = _dot(wo[...], y_s[:, pl.ds(pl.multiple_of(j * step, step), step)], 1, 1)

    @pl.when(j == 0)
    def _():
        acc_s[...] = t

    @pl.when((j > 0) & (j < steps - 1))
    def _():
        acc_s[...] += t

    @pl.when(j == steps - 1)
    def _():
        res_s[...] = (acc_s[...] + t).astype(jnp.bfloat16)
        for p in range(n):
            res_copy(p).start()
        for p in range(n):
            dy_copy(p).wait()
            res_copy(p).wait()


def back_out(rows, pos, at, size, pieces, wo, carry, step=1024):
    nq, d = wo.shape
    n, held = len(pieces), 0 if carry is None else 2
    m = n * size
    return pl.pallas_call(
        functools.partial(_back_out_kernel, at=at, size=size, steps=d // step, n=n, n_alias=held),
        grid_spec=pltpu.PrefetchScalarGridSpec(
            num_scalar_prefetch=1,
            grid=(d // step,),
            in_specs=[pl.BlockSpec((size, d), lambda j, pos: (0, 0))] * n + [pl.BlockSpec((nq, step), lambda j, pos: (0, j))] + [ANY] * held,
            out_specs=[ANY] * 2,
            scratch_shapes=[pltpu.VMEM((m, d), jnp.bfloat16), pltpu.VMEM((nq, m), jnp.float32), pltpu.VMEM((nq, m), jnp.bfloat16),
                            pltpu.SemaphoreType.DMA((n,)), pltpu.SemaphoreType.DMA((n,))],
        ),
        out_shape=[jax.ShapeDtypeStruct((rows, d), jnp.bfloat16), jax.ShapeDtypeStruct((nq, rows), jnp.bfloat16)],
        input_output_aliases={n + 2 + i: i for i in range(held)},
        compiler_params=_params(56 if size == OWN else 40),
        cost_estimate=_cost(2 * m * d * nq, 2 * d * nq),
        name="back_out",
    )(pos, *pieces, wo, *(carry or ()))


def _forward_kernel(q, k, v, pt, ot, vt_s, *, g, scale):
    rows = q.shape[0]
    e = scale * LOG2E

    @pl.when(lax.rem(pl.program_id(0), g) == 0)
    def _():
        vt_s[...] = v[...].T

    later = lax.broadcasted_iota(jnp.int32, (QB, QB), 0) > lax.broadcasted_iota(jnp.int32, (QB, QB), 1)
    scores = lambda i: _dot(k[: (i + 1) * QB], q[i * QB : (i + 1) * QB], 1, 1)
    ahead, at = scores(0), 0
    for i in range(rows // QB):
        end, s = (i + 1) * QB, ahead
        if end < rows:
            ahead = scores(i + 1)
        last = jnp.where(later, HIDDEN, s[end - QB :])
        s = last if i == 0 else jnp.concatenate([s[: end - QB], last], 0)
        top = s.max(axis=0, keepdims=True)
        p = jnp.exp2((s - top) * e)
        p = (p * (1 / p.sum(axis=0, keepdims=True))).astype(jnp.bfloat16)
        pt[0, at : at + end] = p
        ot[:, i * QB : end] = _dot(vt_s[:, :end], p, 1, 0).astype(jnp.bfloat16)
        at += end


def attend(q, k, v):
    rows, nq = q.shape
    heads, kv = nq // HEAD, k.shape[1] // HEAD
    g, nb = heads // kv, rows // QB
    kept = QB * nb * (nb + 1) // 2
    column = pl.BlockSpec((rows, HEAD), lambda h: (0, h))
    shared = pl.BlockSpec((rows, HEAD), lambda h: (0, h // g))
    return pl.pallas_call(
        functools.partial(_forward_kernel, g=g, scale=HEAD**-0.5),
        grid=(heads,),
        in_specs=[column, shared, shared],
        out_specs=[pl.BlockSpec((1, kept, QB), lambda h: (h, 0, 0)), pl.BlockSpec((HEAD, rows), lambda h: (h, 0))],
        out_shape=[jax.ShapeDtypeStruct((heads, kept, QB), jnp.bfloat16), jax.ShapeDtypeStruct((nq, rows), jnp.bfloat16)],
        scratch_shapes=[pltpu.VMEM((HEAD, rows), jnp.bfloat16)],
        compiler_params=_params(58),
        cost_estimate=_cost(8 * heads * kept * QB * HEAD, 2 * heads * kept * QB, heads * kept * QB),
        name="attend",
    )(q, k, v)


def _backward_kernel(pos, q, k, v, dat_0, dat_1, wo_0, wo_1, y0, y1, ot, pt, cos, sin, dy_in, dq, dk, dv, dy_out, kt_s, dk_s, dv_s, y_s, dat_s, sem,
                     *, at_late, at_roles, g, scale):
    rows = q.shape[0]
    step, heads = pl.program_id(0), pl.num_programs(0)
    h, slot = lax.rem(step, g), lax.rem(step, 2)

    def unturn(t, here):
        return (t * cos[here] - pltpu.roll(t, HEAD // 2, 1) * sin[here]).astype(jnp.bfloat16)

    def role(i):
        return pl.ds(pl.multiple_of(pos[at_roles + i] * QB, QB), QB)

    def dy_copy(p):
        return pltpu.make_async_copy((y0, y1)[p], dy_out.at[pl.ds(pos[at_late + p] * PIECE, PIECE)], sem.at[p])

    def keep(slot, some, late):
        dat_s[slot] = some[...]
        for p in range(2):
            here = pl.ds(pl.multiple_of(pos[at_late + p] * PIECE, PIECE), PIECE)
            dat_s[slot, :, here] = late[:, p * PIECE : (p + 1) * PIECE].astype(jnp.bfloat16)

    @pl.when(step == 0)
    def _():
        for p, y in enumerate((y0, y1)):
            dy_copy(p).start()
            y_s[:, p * PIECE : (p + 1) * PIECE] = y[...].T
        keep(0, dat_0, _dot(wo_0[...], y_s[...], 1, 0))

    @pl.when(h == 0)
    def _():
        kt_s[...] = k[...].T
        dk_s[...] = jnp.zeros_like(dk_s)
        dv_s[...] = jnp.zeros_like(dv_s)

    by_weights = lambda i: _dot(v[: (i + 1) * QB], dat_s[slot, :, i * QB : (i + 1) * QB], 1, 0)
    ahead, at = by_weights(0), 0
    late = _dot(wo_1[...], y_s[...], 1, 0)
    for i in range(rows // QB):
        end, dp = (i + 1) * QB, ahead
        if end < rows:
            ahead = by_weights(i + 1)
        here = slice(i * QB, end)
        p = pt[0, at : at + end]
        mine = dat_s[slot, :, here]
        dv_s[:end] += _dot(p, mine, 1, 1)
        delta = (mine.astype(jnp.float32) * ot[:, here].astype(jnp.float32)).sum(axis=0, keepdims=True)
        ds = (p.astype(jnp.float32) * (dp - delta)).astype(jnp.bfloat16)
        dk_s[:end] += _dot(ds, q[here], 1, 0)
        dq[role(i)] = unturn((_dot(kt_s[:, :end], ds, 1, 0) * scale).T, here)
        at += end
    keep(1 - slot, dat_1, late)

    @pl.when(h == g - 1)
    def _():
        for i in range(rows // QB):
            here = slice(i * QB, (i + 1) * QB)
            dk[role(i)] = unturn(dk_s[here] * scale, here)
            dv[role(i)] = dv_s[here].astype(jnp.bfloat16)

    @pl.when(step == heads - 1)
    def _():
        for p in range(2):
            dy_copy(p).wait()


def attend_back(pos, at_late, at_roles, late, q, k, v, dat, wo, dy, ot, pt, cos, sin):
    rows, nq = q.shape
    d = wo.shape[1]
    heads, kv = nq // HEAD, k.shape[1] // HEAD
    g, kept = heads // kv, pt.shape[1]
    column = pl.BlockSpec((rows, HEAD), lambda h, pos: (0, h))
    shared = pl.BlockSpec((rows, HEAD), lambda h, pos: (0, h // g))
    turned = pl.BlockSpec((HEAD, rows), lambda h, pos: (h, 0))
    first = lambda n: pl.BlockSpec((HEAD, n), lambda h, pos: (0, 0))
    following = lambda n: pl.BlockSpec((HEAD, n), lambda h, pos: (jnp.minimum(h + 1, heads - 1), 0))
    table = pl.BlockSpec((rows, HEAD), lambda h, pos: (0, 0))
    piece = pl.BlockSpec((PIECE, d), lambda h, pos: (0, 0))
    return pl.pallas_call(
        functools.partial(_backward_kernel, at_late=at_late, at_roles=at_roles, g=g, scale=HEAD**-0.5),
        grid_spec=pltpu.PrefetchScalarGridSpec(
            num_scalar_prefetch=1,
            grid=(heads,),
            in_specs=[column, shared, shared, first(rows), following(rows), first(d), following(d), piece, piece, turned,
                      pl.BlockSpec((1, kept, QB), lambda h, pos: (h, 0, 0)), table, table, ANY],
            out_specs=[column, shared, shared, ANY],
            scratch_shapes=[pltpu.VMEM((HEAD, rows), jnp.bfloat16), pltpu.VMEM((rows, HEAD), jnp.float32), pltpu.VMEM((rows, HEAD), jnp.float32),
                            pltpu.VMEM((d, 2 * PIECE), jnp.bfloat16), pltpu.VMEM((2, HEAD, rows), jnp.bfloat16), pltpu.SemaphoreType.DMA((2,))],
        ),
        out_shape=[jax.ShapeDtypeStruct(t.shape, jnp.bfloat16) for t in (q, k, v, dy)],
        input_output_aliases={14: 3},
        compiler_params=_params(36),
        cost_estimate=_cost(16 * heads * kept * QB * HEAD + 4 * PIECE * nq * d, 2 * heads * kept * QB + 2 * nq * d),
        name="attend_back",
    )(pos, q, k, v, dat, dat, wo, wo, *late, ot, pt, cos, sin, dy)


def _terms_kernel(q, k, v, a, b, c, stays, leaves, given_s, mine_s, got_s, send_sem, recv_sem):
    j, n = pl.program_id(0), pl.num_programs(0) - 1
    half = 2 * OWN
    me = lax.axis_index("tp")
    partner = {"tp": me + 1 - 2 * lax.rem(me, 2)}

    def hop(i):
        return pltpu.make_async_remote_copy(src_ref=given_s.at[i], dst_ref=got_s.at[i], send_sem=send_sem.at[i], recv_sem=recv_sem.at[i],
                                            device_id=partner, device_id_type=pl.DeviceIdType.MESH)

    @pl.when(j == 0)
    def _():
        barrier = pltpu.get_barrier_semaphore()
        pl.semaphore_signal(barrier, inc=1, device_id=partner, device_id_type=pl.DeviceIdType.MESH)
        pl.semaphore_wait(barrier, 1)

    @pl.when(j < n)
    def _():
        some = lambda rows: sum(_dot(x[rows], w[...], 1, 1) for x, w in ((q, a), (k, b), (v, c)))
        given_s[j] = some(slice(0, half)).astype(jnp.bfloat16)
        hop(j).start()
        mine_s[lax.rem(j, 2)] = some(slice(half, 2 * half))

    @pl.when(j > 0)
    def _():
        hop(j - 1).wait()
        t = mine_s[lax.rem(j - 1, 2)] + got_s[j - 1].astype(jnp.float32)
        stays[...] = t[:OWN]
        leaves[...] = t[OWN:].astype(jnp.bfloat16)


def terms(number, grads, weights, first, width, tile=512):
    base, n = first // tile, width // tile
    depth = sum(t.shape[1] for t in grads)
    one = pl.BlockSpec((OWN, tile), lambda j: (0, jnp.maximum(j - 1, 0)))
    return pl.pallas_call(
        _terms_kernel,
        grid=(n + 1,),
        in_specs=[pl.BlockSpec(t.shape, lambda j: (0, 0)) for t in grads]
        + [pl.BlockSpec((tile, w.shape[1]), lambda j: (base + jnp.minimum(j, n - 1), 0)) for w in weights],
        out_specs=[one, one],
        out_shape=[jax.ShapeDtypeStruct((OWN, width), jnp.float32), jax.ShapeDtypeStruct((OWN, width), jnp.bfloat16)],
        scratch_shapes=[pltpu.VMEM((n, 2 * OWN, tile), jnp.bfloat16), pltpu.VMEM((2, 2 * OWN, tile), jnp.float32),
                        pltpu.VMEM((n, 2 * OWN, tile), jnp.bfloat16), pltpu.SemaphoreType.DMA((n,)), pltpu.SemaphoreType.DMA((n,))],
        compiler_params=_params(48, collective_id=number, has_side_effects=True),
        cost_estimate=_cost(8 * OWN * width * depth, 2 * width * depth),
        name="terms",
    )(*grads, *weights)


def _finish_kernel(*refs, n):
    stays, came, (x, dy, scale, gain, dx, by_gain) = refs[:n], refs[n : 2 * n], refs[2 * n :]
    r, d = scale[:, :1], x.shape[1]
    step = 512

    @pl.when(pl.program_id(0) == 0)
    def _():
        by_gain[...] = jnp.zeros_like(by_gain)

    def parts():
        at = 0
        for a, b in zip(stays, came):
            for c in range(0, a.shape[1], step):
                yield slice(at + c, at + c + step), a[:, c : c + step] + b[:, c : c + step].astype(jnp.float32)
            at += a.shape[1]

    total = 0.0
    for here, g in parts():
        t = g * (x[:, here].astype(jnp.float32) * r)
        by_gain[:, here] += t.sum(0, keepdims=True)
        total = total + t * gain[:, here]
    mean = total.sum(-1, keepdims=True) * (1 / d)
    cut = mean * r * r
    for here, g in parts():
        t = g * gain[:, here] * r - x[:, here].astype(jnp.float32) * cut
        dx[:, here] = (dy[:, here].astype(jnp.float32) + t).astype(jnp.bfloat16)


def finish(stays, came, x, dy, scale, gain, tile=64):
    own, d = x.shape
    some = lambda t: pl.BlockSpec((tile, t.shape[1]), lambda j: (j, 0))
    whole = pl.BlockSpec((1, d), lambda j: (0, 0))
    return pl.pallas_call(
        functools.partial(_finish_kernel, n=len(stays)),
        grid=(own // tile,),
        in_specs=[some(t) for t in (*stays, *came, x, dy, scale)] + [whole],
        out_specs=[some(x), whole],
        out_shape=[jax.ShapeDtypeStruct((own, d), jnp.bfloat16), jax.ShapeDtypeStruct((1, d), jnp.float32)],
        compiler_params=_params(16),
        cost_estimate=_cost(20 * own * d, 14 * own * d),
        name="finish",
    )(*stays, *came, x, dy, scale, gain)


def _by_weights_kernel(nx, dq, dk, dv, ot, dy, oq, ok, ov, oo):
    t = nx[...].T
    for g, o in ((dq, oq), (dk, ok), (dv, ov)):
        o[...] = _dot(t, g[...], 1, 0).astype(jnp.bfloat16)
    oo[...] = _dot(ot[...], dy[...], 1, 0).astype(jnp.bfloat16)


def by_weights(nx, grads, ot, dy, tile=BY_TILE):
    rows, d = nx.shape
    nq = ot.shape[0]
    whole = lambda t: pl.BlockSpec(t.shape, lambda j: (0, 0))
    columns = lambda n: pl.BlockSpec((n, tile), lambda j: (0, j))
    depth = sum(t.shape[1] for t in grads)
    return pl.pallas_call(
        _by_weights_kernel,
        grid=(d // tile,),
        in_specs=[columns(rows), *map(whole, grads), whole(ot), columns(rows)],
        out_specs=[pl.BlockSpec((tile, t.shape[1]), lambda j: (j, 0)) for t in grads] + [columns(nq)],
        out_shape=[jax.ShapeDtypeStruct((d, t.shape[1]), jnp.bfloat16) for t in grads] + [jax.ShapeDtypeStruct((nq, d), jnp.bfloat16)],
        compiler_params=_params(38),
        cost_estimate=_cost(2 * rows * d * (depth + nq), 2 * d * (2 * rows + depth + nq)),
        name="by_weights",
    )(nx, *grads, ot, dy)


ACROSS = [(0, 2), (1, 3), (2, 0), (3, 1)]
BESIDE = [(0, 1), (1, 0), (2, 3), (3, 2)]
CORNER = [(0, 3), (1, 2), (2, 1), (3, 0)]
CHUNKS = (2048, 3072)


def solution(mesh):
    def step(x, dy, gain, wq, wk, wv, wo):
        me = lax.axis_index("tp")
        own, _ = x.shape
        rows = 4 * own
        half = HEAD // 2

        def send(t, way):
            return lax.ppermute(t, "tp", way)

        tie = lax.optimization_barrier

        table = []
        for i in range(4):
            role = [i ^ 1, (i + 2) % 4 ^ 1, i, (i + 2) % 4]
            n = own // PIECE
            table.append([role[2], role[0], role[3], role[1]] + [n * role[b] + p for p in range(n) for b in (3, 1)] + [role.index(b) for b in range(4)])
        pos = lax.dynamic_index_in_dim(jnp.array(table, jnp.int32), me, 0, keepdims=False)
        LOCAL, FAR, FAR_PIECES = 0, 2, 4
        ROLES = FAR_PIECES + 2 * (own // PIECE)

        xp = send(x, BESIDE)
        xa = send(x, ACROSS)
        ya = [send(dy[a : a + PIECE], ACROSS) for a in range(0, own, PIECE)]
        yp = send(dy, BESIDE)

        place = jnp.arange(rows)
        angle = place.astype(jnp.float32)[:, None] * THETA ** (-jnp.arange(half, dtype=jnp.float32) / half)
        cos, sin = jnp.cos(angle), jnp.sin(angle)
        cos, sin = jnp.concatenate([cos, cos], 1), jnp.concatenate([-sin, sin], 1)

        row_gain = gain[None]
        near = project(rows, pos, LOCAL, (2, 0), (x, xp), row_gain, cos, sin, wq, wk, wv, None)
        pos_1, near = tie((pos, near))
        back = back_out(rows, pos_1, LOCAL, own, (dy, yp), wo, None)
        xa, near, back = tie((xa, near, back))
        wide, back = tie((x, back))
        wide = wide.astype(jnp.float32)
        scale = jnp.broadcast_to(lax.rsqrt(jnp.mean(wide * wide, -1, keepdims=True) + 1e-6), (own, HEAD))
        nx, q, k, v = project(rows, pos, FAR, (3, 1), (xa, send(xa, BESIDE)), row_gain, cos, sin, wq, wk, wv, near)
        pt, ot = attend(q, k, v)
        pt, ot, ya[0], back = tie((pt, ot, ya[0], back))
        back = back_out(rows, pos, FAR_PIECES, PIECE, (ya[0], send(ya[0], BESIDE)), wo, back)
        last, (dy_all, dat) = tie((ya[1], back))
        *grads, dy_all = attend_back(pos, FAR_PIECES + 2, ROLES, (last, send(last, BESIDE)), q, k, v, dat, wo, dy_all, ot, pt, cos, sin)

        weights = (wq, wk, wv)
        first, kept, sent = 0, [], []
        for c, width in enumerate(CHUNKS):
            stays, leaves = terms(c, grads, weights, first, width)
            stays, leaves, grads = tie((stays, leaves, grads))
            kept.append(stays)
            sent.append(send(leaves, ACROSS))
            first += width
        nx, leaves = tie((nx, leaves))
        *by_qkv, by_wo = by_weights(nx, grads, ot, dy_all)
        sent, by_wo = tie((sent, by_wo))
        by_x, by_gain = finish(kept, sent, x, dy, scale, gain.astype(jnp.float32)[None])
        by_gain = by_gain + send(by_gain, BESIDE) + (send(by_gain, ACROSS) + send(by_gain, CORNER))
        return (by_x, by_gain, *by_qkv, by_wo)

    tokens, columns = P(("dp", "tp"), None), P(None, "tp")

    return jax.shard_map(
        step,
        mesh=mesh,
        in_specs=(tokens, tokens, P(None), columns, columns, columns, P("tp", None)),
        out_specs=(tokens, P("dp", None), P("dp", "tp"), P("dp", "tp"), P("dp", "tp"), P(("dp", "tp"), None)),
        check_vma=False,
    )
```

```python
import functools

import jax
import jax.numpy as jnp
from jax import lax
from jax.experimental import pallas as pl
from jax.experimental.pallas import tpu as pltpu
from jax.sharding import PartitionSpec as P


HEAD = 128
THETA = 10000
LOG2E = 1.4426950408889634
HIDDEN = -2e30
OWN = 256
PIECE = 128
QB = 256
TILE = 256
BY_TILE = 512
ANY = pl.BlockSpec(memory_space=pl.ANY)


def _dot(a, b, ca, cb):
    return lax.dot_general(a, b, (((ca,), (cb,)), ((), ())), preferred_element_type=jnp.float32)


def _params(mib, n=1, **rest):
    return pltpu.CompilerParams(dimension_semantics=("arbitrary",) * n, vmem_limit_bytes=mib * 2**20, **rest)


def _cost(flops, nbytes, exps=0):
    return pl.CostEstimate(flops=int(flops), bytes_accessed=int(nbytes), transcendentals=int(exps))


def _project_kernel(pos, x0, x1, gain, c0, c1, s0, s1, wq, wk_any, wv_any, *rest, at, roles, qt, n_alias):
    nx_out, q_out, k_out, v_out, nx_s, wk_s, wv_s, res_s, wsem, nsem, rsem = rest[n_alias:]
    j = pl.program_id(0)

    def nx_copy(p):
        return pltpu.make_async_copy(nx_s.at[pl.ds(p * OWN, OWN)], nx_out.at[pl.ds(roles[p] * OWN, OWN)], nsem.at[p])

    def res_copy(p, slot, out, col):
        return pltpu.make_async_copy(res_s.at[slot, pl.ds(p * OWN, OWN)], out.at[pl.ds(pos[at + p] * OWN, OWN), pl.ds(col, TILE)], rsem.at[slot, p])

    wk_copy = pltpu.make_async_copy(wk_any, wk_s, wsem.at[0])
    wv_copy = pltpu.make_async_copy(wv_any, wv_s, wsem.at[1])

    @pl.when(j == 0)
    def _():
        wk_copy.start()
        wv_copy.start()
        for p, ref in enumerate((x0, x1)):
            for r in range(0, OWN, 32):
                wide = ref[r : r + 32].astype(jnp.float32)
                scale = lax.rsqrt(jnp.mean(wide * wide, -1, keepdims=True) + 1e-6)
                nx_s[p * OWN + r : p * OWN + r + 32] = (wide * scale * gain[...].astype(jnp.float32)).astype(jnp.bfloat16)
            nx_copy(p).start()

    def turn(t):
        t = t.astype(jnp.bfloat16).astype(jnp.float32)
        cos = jnp.concatenate([c0[...], c1[...]], 0)
        sin = jnp.concatenate([s0[...], s1[...]], 0)
        heads = [t[:, h : h + HEAD] for h in range(0, TILE, HEAD)]
        return jnp.concatenate([h * cos + pltpu.roll(h, HEAD // 2, 1) * sin for h in heads], 1)

    slot = lax.rem(j, 2)

    @pl.when(j < qt)
    def _():
        @pl.when(j >= 2)
        def _():
            for p in range(2):
                res_copy(p, slot, q_out, pl.multiple_of((j - 2) * TILE, TILE)).wait()

        res_s[slot] = turn(_dot(nx_s[...], wq[...], 1, 0)).astype(jnp.bfloat16)
        for p in range(2):
            res_copy(p, slot, q_out, pl.multiple_of(j * TILE, TILE)).start()

    @pl.when(j == qt)
    def _():
        wk_copy.wait()
        res_s[2] = turn(_dot(nx_s[...], wk_s[...], 1, 0)).astype(jnp.bfloat16)
        for p in range(2):
            res_copy(p, 2, k_out, 0).start()

    @pl.when(j == qt + 1)
    def _():
        wv_copy.wait()
        res_s[3] = _dot(nx_s[...], wv_s[...], 1, 0).astype(jnp.bfloat16)
        for p in range(2):
            res_copy(p, 3, v_out, 0).start()
        for p in range(2):
            nx_copy(p).wait()
            res_copy(p, (qt - 2) % 2, q_out, (qt - 2) * TILE).wait()
            res_copy(p, (qt - 1) % 2, q_out, (qt - 1) * TILE).wait()
            res_copy(p, 2, k_out, 0).wait()
            res_copy(p, 3, v_out, 0).wait()


def project(rows, pos, at, roles, pieces, gain, cos, sin, wq, wk, wv, carry):
    d, nq = wq.shape
    nkv = wk.shape[1]
    qt = nq // TILE
    piece = pl.BlockSpec((OWN, d), lambda j, pos: (0, 0))
    table = lambda p: pl.BlockSpec((OWN, HEAD), lambda j, pos, p=p: (pos[at + p], 0))
    n = 0 if carry is None else 4
    m = 2 * OWN
    return pl.pallas_call(
        functools.partial(_project_kernel, at=at, roles=roles, qt=qt, n_alias=n),
        grid_spec=pltpu.PrefetchScalarGridSpec(
            num_scalar_prefetch=1,
            grid=(qt + 2,),
            in_specs=[piece, piece, pl.BlockSpec((1, d), lambda j, pos: (0, 0)), table(0), table(1), table(0), table(1),
                      pl.BlockSpec((d, TILE), lambda j, pos: (0, jnp.minimum(j, qt - 1))), ANY, ANY] + [ANY] * n,
            out_specs=[ANY] * 4,
            scratch_shapes=[pltpu.VMEM((m, d), jnp.bfloat16), pltpu.VMEM((d, nkv), jnp.bfloat16), pltpu.VMEM((d, nkv), jnp.bfloat16),
                            pltpu.VMEM((4, m, TILE), jnp.bfloat16), pltpu.SemaphoreType.DMA((2,)), pltpu.SemaphoreType.DMA((2,)),
                            pltpu.SemaphoreType.DMA((4, 2))],
        ),
        out_shape=[jax.ShapeDtypeStruct((rows, w), jnp.bfloat16) for w in (d, nq, nkv, nkv)],
        input_output_aliases={11 + i: i for i in range(n)},
        compiler_params=_params(60),
        cost_estimate=_cost(2 * m * d * (nq + 2 * nkv), 2 * d * (nq + 2 * nkv)),
        name="project",
    )(pos, *pieces, gain, cos, cos, sin, sin, wq, wk, wv, *(carry or ()))


def _back_out_kernel(pos, *refs, at, size, steps, n, n_alias):
    ys, wo = refs[:n], refs[n]
    dy_out, da_out, y_s, acc_s, res_s, nsem, rsem = refs[n + 1 + n_alias :]
    j = pl.program_id(0)
    step = wo.shape[1]

    def dy_copy(p):
        return pltpu.make_async_copy(y_s.at[pl.ds(p * size, size)], dy_out.at[pl.ds(pos[at + p] * size, size)], nsem.at[p])

    def res_copy(p):
        return pltpu.make_async_copy(res_s.at[:, pl.ds(p * size, size)], da_out.at[:, pl.ds(pl.multiple_of(pos[at + p] * size, size), size)], rsem.at[p])

    @pl.when(j == 0)
    def _():
        for p, ref in enumerate(ys):
            y_s[p * size : (p + 1) * size] = ref[...]
            dy_copy(p).start()

    t = _dot(wo[...], y_s[:, pl.ds(pl.multiple_of(j * step, step), step)], 1, 1)

    @pl.when(j == 0)
    def _():
        acc_s[...] = t

    @pl.when((j > 0) & (j < steps - 1))
    def _():
        acc_s[...] += t

    @pl.when(j == steps - 1)
    def _():
        res_s[...] = (acc_s[...] + t).astype(jnp.bfloat16)
        for p in range(n):
            res_copy(p).start()
        for p in range(n):
            dy_copy(p).wait()
            res_copy(p).wait()


def back_out(rows, pos, at, size, pieces, wo, carry, step=1024):
    nq, d = wo.shape
    n, held = len(pieces), 0 if carry is None else 2
    m = n * size
    return pl.pallas_call(
        functools.partial(_back_out_kernel, at=at, size=size, steps=d // step, n=n, n_alias=held),
        grid_spec=pltpu.PrefetchScalarGridSpec(
            num_scalar_prefetch=1,
            grid=(d // step,),
            in_specs=[pl.BlockSpec((size, d), lambda j, pos: (0, 0))] * n + [pl.BlockSpec((nq, step), lambda j, pos: (0, j))] + [ANY] * held,
            out_specs=[ANY] * 2,
            scratch_shapes=[pltpu.VMEM((m, d), jnp.bfloat16), pltpu.VMEM((nq, m), jnp.float32), pltpu.VMEM((nq, m), jnp.bfloat16),
                            pltpu.SemaphoreType.DMA((n,)), pltpu.SemaphoreType.DMA((n,))],
        ),
        out_shape=[jax.ShapeDtypeStruct((rows, d), jnp.bfloat16), jax.ShapeDtypeStruct((nq, rows), jnp.bfloat16)],
        input_output_aliases={n + 2 + i: i for i in range(held)},
        compiler_params=_params(56 if size == OWN else 40),
        cost_estimate=_cost(2 * m * d * nq, 2 * d * nq),
        name="back_out",
    )(pos, *pieces, wo, *(carry or ()))


def _forward_kernel(q, k, v, pt, ot, vt_s, *, g, scale):
    rows = q.shape[0]
    e = scale * LOG2E

    @pl.when(lax.rem(pl.program_id(0), g) == 0)
    def _():
        vt_s[...] = v[...].T

    later = lax.broadcasted_iota(jnp.int32, (QB, QB), 0) > lax.broadcasted_iota(jnp.int32, (QB, QB), 1)
    scores = lambda i: _dot(k[: (i + 1) * QB], q[i * QB : (i + 1) * QB], 1, 1)
    ahead, at = scores(0), 0
    for i in range(rows // QB):
        end, s = (i + 1) * QB, ahead
        if end < rows:
            ahead = scores(i + 1)
        last = jnp.where(later, HIDDEN, s[end - QB :])
        s = last if i == 0 else jnp.concatenate([s[: end - QB], last], 0)
        top = s.max(axis=0, keepdims=True)
        p = jnp.exp2((s - top) * e)
        p = (p * (1 / p.sum(axis=0, keepdims=True))).astype(jnp.bfloat16)
        pt[0, at : at + end] = p
        ot[:, i * QB : end] = _dot(vt_s[:, :end], p, 1, 0).astype(jnp.bfloat16)
        at += end


def attend(q, k, v):
    rows, nq = q.shape
    heads, kv = nq // HEAD, k.shape[1] // HEAD
    g, nb = heads // kv, rows // QB
    kept = QB * nb * (nb + 1) // 2
    column = pl.BlockSpec((rows, HEAD), lambda h: (0, h))
    shared = pl.BlockSpec((rows, HEAD), lambda h: (0, h // g))
    return pl.pallas_call(
        functools.partial(_forward_kernel, g=g, scale=HEAD**-0.5),
        grid=(heads,),
        in_specs=[column, shared, shared],
        out_specs=[pl.BlockSpec((1, kept, QB), lambda h: (h, 0, 0)), pl.BlockSpec((HEAD, rows), lambda h: (h, 0))],
        out_shape=[jax.ShapeDtypeStruct((heads, kept, QB), jnp.bfloat16), jax.ShapeDtypeStruct((nq, rows), jnp.bfloat16)],
        scratch_shapes=[pltpu.VMEM((HEAD, rows), jnp.bfloat16)],
        compiler_params=_params(58),
        cost_estimate=_cost(8 * heads * kept * QB * HEAD, 2 * heads * kept * QB, heads * kept * QB),
        name="attend",
    )(q, k, v)


def _backward_kernel(pos, q, k, v, dat_0, dat_1, wo_0, wo_1, y0, y1, ot, pt, cos, sin, dy_in, dq, dk, dv, dy_out, kt_s, dk_s, dv_s, y_s, dat_s, sem,
                     *, at_late, at_roles, g, scale):
    rows = q.shape[0]
    step, heads = pl.program_id(0), pl.num_programs(0)
    h, slot = lax.rem(step, g), lax.rem(step, 2)

    def unturn(t, here):
        return (t * cos[here] - pltpu.roll(t, HEAD // 2, 1) * sin[here]).astype(jnp.bfloat16)

    def role(i):
        return pl.ds(pl.multiple_of(pos[at_roles + i] * QB, QB), QB)

    def dy_copy(p):
        return pltpu.make_async_copy((y0, y1)[p], dy_out.at[pl.ds(pos[at_late + p] * PIECE, PIECE)], sem.at[p])

    def keep(slot, some, late):
        dat_s[slot] = some[...]
        for p in range(2):
            here = pl.ds(pl.multiple_of(pos[at_late + p] * PIECE, PIECE), PIECE)
            dat_s[slot, :, here] = late[:, p * PIECE : (p + 1) * PIECE].astype(jnp.bfloat16)

    @pl.when(step == 0)
    def _():
        for p, y in enumerate((y0, y1)):
            dy_copy(p).start()
            y_s[:, p * PIECE : (p + 1) * PIECE] = y[...].T
        keep(0, dat_0, _dot(wo_0[...], y_s[...], 1, 0))

    @pl.when(h == 0)
    def _():
        kt_s[...] = k[...].T
        dk_s[...] = jnp.zeros_like(dk_s)
        dv_s[...] = jnp.zeros_like(dv_s)

    by_weights = lambda i: _dot(v[: (i + 1) * QB], dat_s[slot, :, i * QB : (i + 1) * QB], 1, 0)
    ahead, at = by_weights(0), 0
    late = _dot(wo_1[...], y_s[...], 1, 0)
    for i in range(rows // QB):
        end, dp = (i + 1) * QB, ahead
        if end < rows:
            ahead = by_weights(i + 1)
        here = slice(i * QB, end)
        p = pt[0, at : at + end]
        mine = dat_s[slot, :, here]
        dv_s[:end] += _dot(p, mine, 1, 1)
        delta = (mine.astype(jnp.float32) * ot[:, here].astype(jnp.float32)).sum(axis=0, keepdims=True)
        ds = (p.astype(jnp.float32) * (dp - delta)).astype(jnp.bfloat16)
        dk_s[:end] += _dot(ds, q[here], 1, 0)
        dq[role(i)] = unturn((_dot(kt_s[:, :end], ds, 1, 0) * scale).T, here)
        at += end
    keep(1 - slot, dat_1, late)

    @pl.when(h == g - 1)
    def _():
        for i in range(rows // QB):
            here = slice(i * QB, (i + 1) * QB)
            dk[role(i)] = unturn(dk_s[here] * scale, here)
            dv[role(i)] = dv_s[here].astype(jnp.bfloat16)

    @pl.when(step == heads - 1)
    def _():
        for p in range(2):
            dy_copy(p).wait()


def attend_back(pos, at_late, at_roles, late, q, k, v, dat, wo, dy, ot, pt, cos, sin):
    rows, nq = q.shape
    d = wo.shape[1]
    heads, kv = nq // HEAD, k.shape[1] // HEAD
    g, kept = heads // kv, pt.shape[1]
    column = pl.BlockSpec((rows, HEAD), lambda h, pos: (0, h))
    shared = pl.BlockSpec((rows, HEAD), lambda h, pos: (0, h // g))
    turned = pl.BlockSpec((HEAD, rows), lambda h, pos: (h, 0))
    first = lambda n: pl.BlockSpec((HEAD, n), lambda h, pos: (0, 0))
    following = lambda n: pl.BlockSpec((HEAD, n), lambda h, pos: (jnp.minimum(h + 1, heads - 1), 0))
    table = pl.BlockSpec((rows, HEAD), lambda h, pos: (0, 0))
    piece = pl.BlockSpec((PIECE, d), lambda h, pos: (0, 0))
    return pl.pallas_call(
        functools.partial(_backward_kernel, at_late=at_late, at_roles=at_roles, g=g, scale=HEAD**-0.5),
        grid_spec=pltpu.PrefetchScalarGridSpec(
            num_scalar_prefetch=1,
            grid=(heads,),
            in_specs=[column, shared, shared, first(rows), following(rows), first(d), following(d), piece, piece, turned,
                      pl.BlockSpec((1, kept, QB), lambda h, pos: (h, 0, 0)), table, table, ANY],
            out_specs=[column, shared, shared, ANY],
            scratch_shapes=[pltpu.VMEM((HEAD, rows), jnp.bfloat16), pltpu.VMEM((rows, HEAD), jnp.float32), pltpu.VMEM((rows, HEAD), jnp.float32),
                            pltpu.VMEM((d, 2 * PIECE), jnp.bfloat16), pltpu.VMEM((2, HEAD, rows), jnp.bfloat16), pltpu.SemaphoreType.DMA((2,))],
        ),
        out_shape=[jax.ShapeDtypeStruct(t.shape, jnp.bfloat16) for t in (q, k, v, dy)],
        input_output_aliases={14: 3},
        compiler_params=_params(40),
        cost_estimate=_cost(16 * heads * kept * QB * HEAD + 4 * PIECE * nq * d, 2 * heads * kept * QB + 2 * nq * d),
        name="attend_back",
    )(pos, q, k, v, dat, dat, wo, wo, *late, ot, pt, cos, sin, dy)


def _terms_kernel(q, k, v, a, b, c, stays, leaves, given_s, mine_s, got_s, send_sem, recv_sem):
    j, n = pl.program_id(0), pl.num_programs(0) - 1
    half = 2 * OWN
    me = lax.axis_index("tp")
    partner = {"tp": me + 1 - 2 * lax.rem(me, 2)}

    def hop(i):
        return pltpu.make_async_remote_copy(src_ref=given_s.at[i], dst_ref=got_s.at[i], send_sem=send_sem.at[i], recv_sem=recv_sem.at[i],
                                            device_id=partner, device_id_type=pl.DeviceIdType.MESH)

    @pl.when(j == 0)
    def _():
        barrier = pltpu.get_barrier_semaphore()
        pl.semaphore_signal(barrier, inc=1, device_id=partner, device_id_type=pl.DeviceIdType.MESH)
        pl.semaphore_wait(barrier, 1)

    @pl.when(j < n)
    def _():
        some = lambda rows: sum(_dot(x[rows], w[...], 1, 1) for x, w in ((q, a), (k, b), (v, c)))
        given_s[j] = some(slice(0, half)).astype(jnp.bfloat16)
        hop(j).start()
        mine_s[lax.rem(j, 2)] = some(slice(half, 2 * half))

    @pl.when(j > 0)
    def _():
        hop(j - 1).wait()
        t = mine_s[lax.rem(j - 1, 2)] + got_s[j - 1].astype(jnp.float32)
        stays[...] = t[:OWN]
        leaves[...] = t[OWN:].astype(jnp.bfloat16)


def terms(number, grads, weights, first, width, tile=512):
    base, n = first // tile, width // tile
    depth = sum(t.shape[1] for t in grads)
    one = pl.BlockSpec((OWN, tile), lambda j: (0, jnp.maximum(j - 1, 0)))
    return pl.pallas_call(
        _terms_kernel,
        grid=(n + 1,),
        in_specs=[pl.BlockSpec(t.shape, lambda j: (0, 0)) for t in grads]
        + [pl.BlockSpec((tile, w.shape[1]), lambda j: (base + jnp.minimum(j, n - 1), 0)) for w in weights],
        out_specs=[one, one],
        out_shape=[jax.ShapeDtypeStruct((OWN, width), jnp.float32), jax.ShapeDtypeStruct((OWN, width), jnp.bfloat16)],
        scratch_shapes=[pltpu.VMEM((n, 2 * OWN, tile), jnp.bfloat16), pltpu.VMEM((2, 2 * OWN, tile), jnp.float32),
                        pltpu.VMEM((n, 2 * OWN, tile), jnp.bfloat16), pltpu.SemaphoreType.DMA((n,)), pltpu.SemaphoreType.DMA((n,))],
        compiler_params=_params(52, collective_id=number, has_side_effects=True),
        cost_estimate=_cost(8 * OWN * width * depth, 2 * width * depth),
        name="terms",
    )(*grads, *weights)


def _parts(stays, came, step=512):
    at = 0
    for a, b in zip(stays, came):
        for c in range(0, a.shape[1], step):
            yield slice(at + c, at + c + step), a[:, c : c + step] + b[:, c : c + step].astype(jnp.float32)
        at += a.shape[1]


def _sums_kernel(*refs, n):
    stays, came, (x, scale, gain, by_gain, cut) = refs[:n], refs[n : 2 * n], refs[2 * n :]
    r = scale[:, :1]

    @pl.when(pl.program_id(0) == 0)
    def _():
        by_gain[...] = jnp.zeros_like(by_gain)

    total = 0.0
    for here, g in _parts(stays, came):
        t = g * (x[:, here].astype(jnp.float32) * r)
        by_gain[:, here] += t.sum(0, keepdims=True)
        total = total + t * gain[:, here]
    cut[...] = jnp.broadcast_to(total.sum(-1, keepdims=True) * (1 / x.shape[1]) * r * r, cut.shape)


def _finish_kernel(*refs, n):
    stays, came, (x, dy, scale, cut, gain, dx) = refs[:n], refs[n : 2 * n], refs[2 * n :]
    r, c = scale[:, :1], cut[:, :1]
    for here, g in _parts(stays, came):
        t = g * gain[:, here] * r - x[:, here].astype(jnp.float32) * c
        dx[:, here] = (dy[:, here].astype(jnp.float32) + t).astype(jnp.bfloat16)


def _by_rows(kernel, rows, gain, outs, tile=64):
    own, d = rows[-1].shape[0], gain.shape[1]
    some = lambda t: pl.BlockSpec((tile, t.shape[1]), lambda j: (j, 0))
    whole = pl.BlockSpec((1, d), lambda j: (0, 0))
    return pl.pallas_call(
        kernel,
        grid=(own // tile,),
        in_specs=[*map(some, rows), whole],
        out_specs=[some(t) if t.shape[0] > 1 else whole for t in outs],
        out_shape=outs,
        compiler_params=_params(16),
        cost_estimate=_cost(10 * own * d, 10 * own * d),
    )(*rows, gain)


def _by_weights_kernel(nx, dq, dk, dv, ot, dy, oq, ok, ov, oo):
    t = nx[...].T
    for g, o in ((dq, oq), (dk, ok), (dv, ov)):
        o[...] = _dot(t, g[...], 1, 0).astype(jnp.bfloat16)
    oo[...] = _dot(ot[...], dy[...], 1, 0).astype(jnp.bfloat16)


def by_weights(nx, grads, ot, dy, tile=BY_TILE):
    rows, d = nx.shape
    nq = ot.shape[0]
    whole = lambda t: pl.BlockSpec(t.shape, lambda j: (0, 0))
    columns = lambda n: pl.BlockSpec((n, tile), lambda j: (0, j))
    depth = sum(t.shape[1] for t in grads)
    return pl.pallas_call(
        _by_weights_kernel,
        grid=(d // tile,),
        in_specs=[columns(rows), *map(whole, grads), whole(ot), columns(rows)],
        out_specs=[pl.BlockSpec((tile, t.shape[1]), lambda j: (j, 0)) for t in grads] + [columns(nq)],
        out_shape=[jax.ShapeDtypeStruct((d, t.shape[1]), jnp.bfloat16) for t in grads] + [jax.ShapeDtypeStruct((nq, d), jnp.bfloat16)],
        compiler_params=_params(38),
        cost_estimate=_cost(2 * rows * d * (depth + nq), 2 * d * (2 * rows + depth + nq)),
        name="by_weights",
    )(nx, *grads, ot, dy)


ACROSS = [(0, 2), (1, 3), (2, 0), (3, 1)]
BESIDE = [(0, 1), (1, 0), (2, 3), (3, 2)]
CORNER = [(0, 3), (1, 2), (2, 1), (3, 0)]
CHUNKS = (2048, 3072)


def solution(mesh):
    def step(x, dy, gain, wq, wk, wv, wo):
        me = lax.axis_index("tp")
        own, d = x.shape
        rows = 4 * own
        half = HEAD // 2

        def send(t, way):
            return lax.ppermute(t, "tp", way)

        tie = lax.optimization_barrier

        table = []
        for i in range(4):
            role = [i ^ 1, (i + 2) % 4 ^ 1, i, (i + 2) % 4]
            n = own // PIECE
            table.append([role[2], role[0], role[3], role[1]] + [n * role[b] + p for p in range(n) for b in (3, 1)] + [role.index(b) for b in range(4)])
        pos = lax.dynamic_index_in_dim(jnp.array(table, jnp.int32), me, 0, keepdims=False)
        LOCAL, FAR, FAR_PIECES = 0, 2, 4
        ROLES = FAR_PIECES + 2 * (own // PIECE)

        xp = send(x, BESIDE)
        xa = send(x, ACROSS)
        ya = [send(dy[a : a + PIECE], ACROSS) for a in range(0, own, PIECE)]
        yp = send(dy, BESIDE)

        place = jnp.arange(rows)
        angle = place.astype(jnp.float32)[:, None] * THETA ** (-jnp.arange(half, dtype=jnp.float32) / half)
        cos, sin = jnp.cos(angle), jnp.sin(angle)
        cos, sin = jnp.concatenate([cos, cos], 1), jnp.concatenate([-sin, sin], 1)

        row_gain = gain[None]
        near = project(rows, pos, LOCAL, (2, 0), (x, xp), row_gain, cos, sin, wq, wk, wv, None)
        pos_1, near = tie((pos, near))
        back = back_out(rows, pos_1, LOCAL, own, (dy, yp), wo, None)
        xa, near, back = tie((xa, near, back))
        wide, back = tie((x, back))
        wide = wide.astype(jnp.float32)
        scale = jnp.broadcast_to(lax.rsqrt(jnp.mean(wide * wide, -1, keepdims=True) + 1e-6), (own, HEAD))
        nx, q, k, v = project(rows, pos, FAR, (3, 1), (xa, send(xa, BESIDE)), row_gain, cos, sin, wq, wk, wv, near)
        pt, ot = attend(q, k, v)
        pt, ot, ya[0], back = tie((pt, ot, ya[0], back))
        back = back_out(rows, pos, FAR_PIECES, PIECE, (ya[0], send(ya[0], BESIDE)), wo, back)
        last, (dy_all, dat) = tie((ya[1], back))
        *grads, dy_all = attend_back(pos, FAR_PIECES + 2, ROLES, (last, send(last, BESIDE)), q, k, v, dat, wo, dy_all, ot, pt, cos, sin)

        weights = (wq, wk, wv)
        first, kept, sent = 0, [], []
        for c, width in enumerate(CHUNKS):
            stays, leaves = terms(c, grads, weights, first, width)
            stays, leaves, grads = tie((stays, leaves, grads))
            kept.append(stays)
            sent.append(send(leaves, ACROSS))
            first += width
        nx, leaves = tie((nx, leaves))
        *by_qkv, by_wo = by_weights(nx, grads, ot, dy_all)
        sent, by_wo = tie((sent, by_wo))
        wide_gain, n = gain.astype(jnp.float32)[None], len(CHUNKS)
        by_gain, cut = _by_rows(functools.partial(_sums_kernel, n=n), (*kept, *sent, x, scale), wide_gain,
                                [jax.ShapeDtypeStruct((1, d), jnp.float32), jax.ShapeDtypeStruct((own, HEAD), jnp.float32)])
        others = [send(by_gain, way) for way in (BESIDE, ACROSS, CORNER)]
        by_x, = _by_rows(functools.partial(_finish_kernel, n=n), (*kept, *sent, x, dy, scale, cut), wide_gain,
                         [jax.ShapeDtypeStruct((own, d), jnp.bfloat16)])
        by_gain = by_gain + others[0] + (others[1] + others[2])
        return (by_x, by_gain, *by_qkv, by_wo)

    tokens, columns = P(("dp", "tp"), None), P(None, "tp")

    return jax.shard_map(
        step,
        mesh=mesh,
        in_specs=(tokens, tokens, P(None), columns, columns, columns, P("tp", None)),
        out_specs=(tokens, P("dp", None), P("dp", "tp"), P("dp", "tp"), P("dp", "tp"), P(("dp", "tp"), None)),
        check_vma=False,
    )
```

```python
import functools

import jax
import jax.numpy as jnp
from jax import lax
from jax.experimental import pallas as pl
from jax.experimental.pallas import tpu as pltpu
from jax.sharding import PartitionSpec as P


HEAD = 128
THETA = 10000
LOG2E = 1.4426950408889634
HIDDEN = -2e30
OWN = 256
PIECE = 128
QB = 256
TILE = 256
BY_TILE = 512
ANY = pl.BlockSpec(memory_space=pl.ANY)


def _dot(a, b, ca, cb):
    return lax.dot_general(a, b, (((ca,), (cb,)), ((), ())), preferred_element_type=jnp.float32)


def _params(mib, n=1, **rest):
    return pltpu.CompilerParams(dimension_semantics=("arbitrary",) * n, vmem_limit_bytes=mib * 2**20, **rest)


def _cost(flops, nbytes, exps=0):
    return pl.CostEstimate(flops=int(flops), bytes_accessed=int(nbytes), transcendentals=int(exps))


def _project_kernel(pos, x0, x1, gain, c0, c1, s0, s1, wq, wk_any, wv_any, *rest, at, roles, qt, n_alias):
    nx_out, q_out, k_out, v_out, nx_s, wk_s, wv_s, res_s, wsem, nsem, rsem = rest[n_alias:]
    j = pl.program_id(0)

    def nx_copy(p):
        return pltpu.make_async_copy(nx_s.at[pl.ds(p * OWN, OWN)], nx_out.at[pl.ds(roles[p] * OWN, OWN)], nsem.at[p])

    def res_copy(p, slot, out, col):
        return pltpu.make_async_copy(res_s.at[slot, pl.ds(p * OWN, OWN)], out.at[pl.ds(pos[at + p] * OWN, OWN), pl.ds(col, TILE)], rsem.at[slot, p])

    wk_copy = pltpu.make_async_copy(wk_any, wk_s, wsem.at[0])
    wv_copy = pltpu.make_async_copy(wv_any, wv_s, wsem.at[1])

    @pl.when(j == 0)
    def _():
        wk_copy.start()
        wv_copy.start()
        for p, ref in enumerate((x0, x1)):
            for r in range(0, OWN, 32):
                wide = ref[r : r + 32].astype(jnp.float32)
                scale = lax.rsqrt(jnp.mean(wide * wide, -1, keepdims=True) + 1e-6)
                nx_s[p * OWN + r : p * OWN + r + 32] = (wide * scale * gain[...].astype(jnp.float32)).astype(jnp.bfloat16)
            nx_copy(p).start()

    def turn(t):
        t = t.astype(jnp.bfloat16).astype(jnp.float32)
        cos = jnp.concatenate([c0[...], c1[...]], 0)
        sin = jnp.concatenate([s0[...], s1[...]], 0)
        heads = [t[:, h : h + HEAD] for h in range(0, TILE, HEAD)]
        return jnp.concatenate([h * cos + pltpu.roll(h, HEAD // 2, 1) * sin for h in heads], 1)

    slot = lax.rem(j, 2)

    @pl.when(j < qt)
    def _():
        @pl.when(j >= 2)
        def _():
            for p in range(2):
                res_copy(p, slot, q_out, pl.multiple_of((j - 2) * TILE, TILE)).wait()

        res_s[slot] = turn(_dot(nx_s[...], wq[...], 1, 0)).astype(jnp.bfloat16)
        for p in range(2):
            res_copy(p, slot, q_out, pl.multiple_of(j * TILE, TILE)).start()

    @pl.when(j == qt)
    def _():
        wk_copy.wait()
        res_s[2] = turn(_dot(nx_s[...], wk_s[...], 1, 0)).astype(jnp.bfloat16)
        for p in range(2):
            res_copy(p, 2, k_out, 0).start()

    @pl.when(j == qt + 1)
    def _():
        wv_copy.wait()
        res_s[3] = _dot(nx_s[...], wv_s[...], 1, 0).astype(jnp.bfloat16)
        for p in range(2):
            res_copy(p, 3, v_out, 0).start()
        for p in range(2):
            nx_copy(p).wait()
            res_copy(p, (qt - 2) % 2, q_out, (qt - 2) * TILE).wait()
            res_copy(p, (qt - 1) % 2, q_out, (qt - 1) * TILE).wait()
            res_copy(p, 2, k_out, 0).wait()
            res_copy(p, 3, v_out, 0).wait()


def project(rows, pos, at, roles, pieces, gain, cos, sin, wq, wk, wv, carry):
    d, nq = wq.shape
    nkv = wk.shape[1]
    qt = nq // TILE
    piece = pl.BlockSpec((OWN, d), lambda j, pos: (0, 0))
    table = lambda p: pl.BlockSpec((OWN, HEAD), lambda j, pos, p=p: (pos[at + p], 0))
    n = 0 if carry is None else 4
    m = 2 * OWN
    return pl.pallas_call(
        functools.partial(_project_kernel, at=at, roles=roles, qt=qt, n_alias=n),
        grid_spec=pltpu.PrefetchScalarGridSpec(
            num_scalar_prefetch=1,
            grid=(qt + 2,),
            in_specs=[piece, piece, pl.BlockSpec((1, d), lambda j, pos: (0, 0)), table(0), table(1), table(0), table(1),
                      pl.BlockSpec((d, TILE), lambda j, pos: (0, jnp.minimum(j, qt - 1))), ANY, ANY] + [ANY] * n,
            out_specs=[ANY] * 4,
            scratch_shapes=[pltpu.VMEM((m, d), jnp.bfloat16), pltpu.VMEM((d, nkv), jnp.bfloat16), pltpu.VMEM((d, nkv), jnp.bfloat16),
                            pltpu.VMEM((4, m, TILE), jnp.bfloat16), pltpu.SemaphoreType.DMA((2,)), pltpu.SemaphoreType.DMA((2,)),
                            pltpu.SemaphoreType.DMA((4, 2))],
        ),
        out_shape=[jax.ShapeDtypeStruct((rows, w), jnp.bfloat16) for w in (d, nq, nkv, nkv)],
        input_output_aliases={11 + i: i for i in range(n)},
        compiler_params=_params(60),
        cost_estimate=_cost(2 * m * d * (nq + 2 * nkv), 2 * d * (nq + 2 * nkv)),
        name="project",
    )(pos, *pieces, gain, cos, cos, sin, sin, wq, wk, wv, *(carry or ()))


def _back_out_kernel(pos, *refs, at, size, steps, n, n_alias):
    ys, wo = refs[:n], refs[n]
    dy_out, da_out, y_s, acc_s, res_s, nsem, rsem = refs[n + 1 + n_alias :]
    j = pl.program_id(0)
    step = wo.shape[1]

    def dy_copy(p):
        return pltpu.make_async_copy(y_s.at[pl.ds(p * size, size)], dy_out.at[pl.ds(pos[at + p] * size, size)], nsem.at[p])

    def res_copy(p):
        return pltpu.make_async_copy(res_s.at[:, pl.ds(p * size, size)], da_out.at[:, pl.ds(pl.multiple_of(pos[at + p] * size, size), size)], rsem.at[p])

    @pl.when(j == 0)
    def _():
        for p, ref in enumerate(ys):
            y_s[p * size : (p + 1) * size] = ref[...]
            dy_copy(p).start()

    t = _dot(wo[...], y_s[:, pl.ds(pl.multiple_of(j * step, step), step)], 1, 1)

    @pl.when(j == 0)
    def _():
        acc_s[...] = t

    @pl.when((j > 0) & (j < steps - 1))
    def _():
        acc_s[...] += t

    @pl.when(j == steps - 1)
    def _():
        res_s[...] = (acc_s[...] + t).astype(jnp.bfloat16)
        for p in range(n):
            res_copy(p).start()
        for p in range(n):
            dy_copy(p).wait()
            res_copy(p).wait()


def back_out(rows, pos, at, size, pieces, wo, carry, step=1024):
    nq, d = wo.shape
    n, held = len(pieces), 0 if carry is None else 2
    m = n * size
    return pl.pallas_call(
        functools.partial(_back_out_kernel, at=at, size=size, steps=d // step, n=n, n_alias=held),
        grid_spec=pltpu.PrefetchScalarGridSpec(
            num_scalar_prefetch=1,
            grid=(d // step,),
            in_specs=[pl.BlockSpec((size, d), lambda j, pos: (0, 0))] * n + [pl.BlockSpec((nq, step), lambda j, pos: (0, j))] + [ANY] * held,
            out_specs=[ANY] * 2,
            scratch_shapes=[pltpu.VMEM((m, d), jnp.bfloat16), pltpu.VMEM((nq, m), jnp.float32), pltpu.VMEM((nq, m), jnp.bfloat16),
                            pltpu.SemaphoreType.DMA((n,)), pltpu.SemaphoreType.DMA((n,))],
        ),
        out_shape=[jax.ShapeDtypeStruct((rows, d), jnp.bfloat16), jax.ShapeDtypeStruct((nq, rows), jnp.bfloat16)],
        input_output_aliases={n + 2 + i: i for i in range(held)},
        compiler_params=_params(56 if size == OWN else 40),
        cost_estimate=_cost(2 * m * d * nq, 2 * d * nq),
        name="back_out",
    )(pos, *pieces, wo, *(carry or ()))


def _forward_kernel(q, k, v, pt, ot, vt_s, *, g, scale):
    rows = q.shape[0]
    e = scale * LOG2E

    @pl.when(lax.rem(pl.program_id(0), g) == 0)
    def _():
        vt_s[...] = v[...].T

    later = lax.broadcasted_iota(jnp.int32, (QB, QB), 0) > lax.broadcasted_iota(jnp.int32, (QB, QB), 1)
    scores = lambda i: _dot(k[: (i + 1) * QB], q[i * QB : (i + 1) * QB], 1, 1)
    ahead, at = scores(0), 0
    for i in range(rows // QB):
        end, s = (i + 1) * QB, ahead
        if end < rows:
            ahead = scores(i + 1)
        last = jnp.where(later, HIDDEN, s[end - QB :])
        s = last if i == 0 else jnp.concatenate([s[: end - QB], last], 0)
        top = s.max(axis=0, keepdims=True)
        p = jnp.exp2((s - top) * e)
        p = (p * (1 / p.sum(axis=0, keepdims=True))).astype(jnp.bfloat16)
        pt[0, at : at + end] = p
        ot[:, i * QB : end] = _dot(vt_s[:, :end], p, 1, 0).astype(jnp.bfloat16)
        at += end


def attend(q, k, v):
    rows, nq = q.shape
    heads, kv = nq // HEAD, k.shape[1] // HEAD
    g, nb = heads // kv, rows // QB
    kept = QB * nb * (nb + 1) // 2
    column = pl.BlockSpec((rows, HEAD), lambda h: (0, h))
    shared = pl.BlockSpec((rows, HEAD), lambda h: (0, h // g))
    return pl.pallas_call(
        functools.partial(_forward_kernel, g=g, scale=HEAD**-0.5),
        grid=(heads,),
        in_specs=[column, shared, shared],
        out_specs=[pl.BlockSpec((1, kept, QB), lambda h: (h, 0, 0)), pl.BlockSpec((HEAD, rows), lambda h: (h, 0))],
        out_shape=[jax.ShapeDtypeStruct((heads, kept, QB), jnp.bfloat16), jax.ShapeDtypeStruct((nq, rows), jnp.bfloat16)],
        scratch_shapes=[pltpu.VMEM((HEAD, rows), jnp.bfloat16)],
        compiler_params=_params(58),
        cost_estimate=_cost(8 * heads * kept * QB * HEAD, 2 * heads * kept * QB, heads * kept * QB),
        name="attend",
    )(q, k, v)


def _backward_kernel(pos, q, k, v, dat_0, dat_1, wo_0, wo_1, y0, y1, ot, pt, cos, sin, dy_in, dq, dk, dv, dy_out, kt_s, dk_s, dv_s, y_s, dat_s, sem,
                     *, at_late, at_roles, g, scale):
    rows = q.shape[0]
    step, heads = pl.program_id(0), pl.num_programs(0)
    h, slot = lax.rem(step, g), lax.rem(step, 2)

    def unturn(t, here):
        return (t * cos[here] - pltpu.roll(t, HEAD // 2, 1) * sin[here]).astype(jnp.bfloat16)

    def role(i):
        return pl.ds(pl.multiple_of(pos[at_roles + i] * QB, QB), QB)

    def dy_copy(p):
        return pltpu.make_async_copy((y0, y1)[p], dy_out.at[pl.ds(pos[at_late + p] * PIECE, PIECE)], sem.at[p])

    def keep(slot, some, late):
        dat_s[slot] = some[...]
        for p in range(2):
            here = pl.ds(pl.multiple_of(pos[at_late + p] * PIECE, PIECE), PIECE)
            dat_s[slot, :, here] = late[:, p * PIECE : (p + 1) * PIECE].astype(jnp.bfloat16)

    @pl.when(step == 0)
    def _():
        for p, y in enumerate((y0, y1)):
            dy_copy(p).start()
            y_s[:, p * PIECE : (p + 1) * PIECE] = y[...].T
        keep(0, dat_0, _dot(wo_0[...], y_s[...], 1, 0))

    @pl.when(h == 0)
    def _():
        kt_s[...] = k[...].T
        dk_s[...] = jnp.zeros_like(dk_s)
        dv_s[...] = jnp.zeros_like(dv_s)

    by_weights = lambda i: _dot(v[: (i + 1) * QB], dat_s[slot, :, i * QB : (i + 1) * QB], 1, 0)
    ahead, at = by_weights(0), 0
    late = _dot(wo_1[...], y_s[...], 1, 0)
    for i in range(rows // QB):
        end, dp = (i + 1) * QB, ahead
        if end < rows:
            ahead = by_weights(i + 1)
        here = slice(i * QB, end)
        p = pt[0, at : at + end]
        mine = dat_s[slot, :, here]
        dv_s[:end] += _dot(p, mine, 1, 1)
        delta = (mine.astype(jnp.float32) * ot[:, here].astype(jnp.float32)).sum(axis=0, keepdims=True)
        ds = (p.astype(jnp.float32) * (dp - delta)).astype(jnp.bfloat16)
        dk_s[:end] += _dot(ds, q[here], 1, 0)
        dq[role(i)] = unturn((_dot(kt_s[:, :end], ds, 1, 0) * scale).T, here)
        at += end
    keep(1 - slot, dat_1, late)

    @pl.when(h == g - 1)
    def _():
        for i in range(rows // QB):
            here = slice(i * QB, (i + 1) * QB)
            dk[role(i)] = unturn(dk_s[here] * scale, here)
            dv[role(i)] = dv_s[here].astype(jnp.bfloat16)

    @pl.when(step == heads - 1)
    def _():
        for p in range(2):
            dy_copy(p).wait()


def attend_back(pos, at_late, at_roles, late, q, k, v, dat, wo, dy, ot, pt, cos, sin):
    rows, nq = q.shape
    d = wo.shape[1]
    heads, kv = nq // HEAD, k.shape[1] // HEAD
    g, kept = heads // kv, pt.shape[1]
    column = pl.BlockSpec((rows, HEAD), lambda h, pos: (0, h))
    shared = pl.BlockSpec((rows, HEAD), lambda h, pos: (0, h // g))
    turned = pl.BlockSpec((HEAD, rows), lambda h, pos: (h, 0))
    first = lambda n: pl.BlockSpec((HEAD, n), lambda h, pos: (0, 0))
    following = lambda n: pl.BlockSpec((HEAD, n), lambda h, pos: (jnp.minimum(h + 1, heads - 1), 0))
    table = pl.BlockSpec((rows, HEAD), lambda h, pos: (0, 0))
    piece = pl.BlockSpec((PIECE, d), lambda h, pos: (0, 0))
    return pl.pallas_call(
        functools.partial(_backward_kernel, at_late=at_late, at_roles=at_roles, g=g, scale=HEAD**-0.5),
        grid_spec=pltpu.PrefetchScalarGridSpec(
            num_scalar_prefetch=1,
            grid=(heads,),
            in_specs=[column, shared, shared, first(rows), following(rows), first(d), following(d), piece, piece, turned,
                      pl.BlockSpec((1, kept, QB), lambda h, pos: (h, 0, 0)), table, table, ANY],
            out_specs=[column, shared, shared, ANY],
            scratch_shapes=[pltpu.VMEM((HEAD, rows), jnp.bfloat16), pltpu.VMEM((rows, HEAD), jnp.float32), pltpu.VMEM((rows, HEAD), jnp.float32),
                            pltpu.VMEM((d, 2 * PIECE), jnp.bfloat16), pltpu.VMEM((2, HEAD, rows), jnp.bfloat16), pltpu.SemaphoreType.DMA((2,))],
        ),
        out_shape=[jax.ShapeDtypeStruct(t.shape, jnp.bfloat16) for t in (q, k, v, dy)],
        input_output_aliases={14: 3},
        compiler_params=_params(46),
        cost_estimate=_cost(16 * heads * kept * QB * HEAD + 4 * PIECE * nq * d, 2 * heads * kept * QB + 2 * nq * d),
        name="attend_back",
    )(pos, q, k, v, dat, dat, wo, wo, *late, ot, pt, cos, sin, dy)


def _terms_kernel(q, k, v, a, b, c, stays, leaves, given_s, mine_s, got_s, send_sem, recv_sem):
    j, n = pl.program_id(0), pl.num_programs(0) - 1
    half = 2 * OWN
    me = lax.axis_index("tp")
    partner = {"tp": me + 1 - 2 * lax.rem(me, 2)}

    def hop(i):
        return pltpu.make_async_remote_copy(src_ref=given_s.at[i], dst_ref=got_s.at[i], send_sem=send_sem.at[i], recv_sem=recv_sem.at[i],
                                            device_id=partner, device_id_type=pl.DeviceIdType.MESH)

    @pl.when(j == 0)
    def _():
        barrier = pltpu.get_barrier_semaphore()
        pl.semaphore_signal(barrier, inc=1, device_id=partner, device_id_type=pl.DeviceIdType.MESH)
        pl.semaphore_wait(barrier, 1)

    @pl.when(j < n)
    def _():
        some = lambda rows: sum(_dot(x[rows], w[...], 1, 1) for x, w in ((q, a), (k, b), (v, c)))
        given_s[j] = some(slice(0, half)).astype(jnp.bfloat16)
        hop(j).start()
        mine_s[lax.rem(j, 2)] = some(slice(half, 2 * half))

    @pl.when(j > 0)
    def _():
        hop(j - 1).wait()
        t = mine_s[lax.rem(j - 1, 2)] + got_s[j - 1].astype(jnp.float32)
        stays[...] = t[:OWN]
        leaves[...] = t[OWN:].astype(jnp.bfloat16)


def terms(number, grads, weights, first, width, tile=512):
    base, n = first // tile, width // tile
    depth = sum(t.shape[1] for t in grads)
    one = pl.BlockSpec((OWN, tile), lambda j: (0, jnp.maximum(j - 1, 0)))
    return pl.pallas_call(
        _terms_kernel,
        grid=(n + 1,),
        in_specs=[pl.BlockSpec(t.shape, lambda j: (0, 0)) for t in grads]
        + [pl.BlockSpec((tile, w.shape[1]), lambda j: (base + jnp.minimum(j, n - 1), 0)) for w in weights],
        out_specs=[one, one],
        out_shape=[jax.ShapeDtypeStruct((OWN, width), jnp.float32), jax.ShapeDtypeStruct((OWN, width), jnp.bfloat16)],
        scratch_shapes=[pltpu.VMEM((n, 2 * OWN, tile), jnp.bfloat16), pltpu.VMEM((2, 2 * OWN, tile), jnp.float32),
                        pltpu.VMEM((n, 2 * OWN, tile), jnp.bfloat16), pltpu.SemaphoreType.DMA((n,)), pltpu.SemaphoreType.DMA((n,))],
        compiler_params=_params(52, collective_id=number, has_side_effects=True),
        cost_estimate=_cost(8 * OWN * width * depth, 2 * width * depth),
        name="terms",
    )(*grads, *weights)


def _parts(stays, came, step=512):
    at = 0
    for a, b in zip(stays, came):
        for c in range(0, a.shape[1], step):
            yield slice(at + c, at + c + step), a[:, c : c + step] + b[:, c : c + step].astype(jnp.float32)
        at += a.shape[1]


def _sums_kernel(*refs, n):
    stays, came, (x, scale, gain, by_gain, cut) = refs[:n], refs[n : 2 * n], refs[2 * n :]
    r = scale[:, :1]

    @pl.when(pl.program_id(0) == 0)
    def _():
        by_gain[...] = jnp.zeros_like(by_gain)

    total = 0.0
    for here, g in _parts(stays, came):
        t = g * (x[:, here].astype(jnp.float32) * r)
        by_gain[:, here] += t.sum(0, keepdims=True)
        total = total + t * gain[:, here]
    cut[...] = jnp.broadcast_to(total.sum(-1, keepdims=True) * (1 / x.shape[1]) * r * r, cut.shape)


def _finish_kernel(*refs, n):
    stays, came, (x, dy, scale, cut, gain, dx) = refs[:n], refs[n : 2 * n], refs[2 * n :]
    r, c = scale[:, :1], cut[:, :1]
    for here, g in _parts(stays, came):
        t = g * gain[:, here] * r - x[:, here].astype(jnp.float32) * c
        dx[:, here] = (dy[:, here].astype(jnp.float32) + t).astype(jnp.bfloat16)


def _by_rows(kernel, rows, gain, outs, tile=64):
    own, d = rows[-1].shape[0], gain.shape[1]
    some = lambda t: pl.BlockSpec((tile, t.shape[1]), lambda j: (j, 0))
    whole = pl.BlockSpec((1, d), lambda j: (0, 0))
    return pl.pallas_call(
        kernel,
        grid=(own // tile,),
        in_specs=[*map(some, rows), whole],
        out_specs=[some(t) if t.shape[0] > 1 else whole for t in outs],
        out_shape=outs,
        compiler_params=_params(16),
        cost_estimate=_cost(10 * own * d, 10 * own * d),
    )(*rows, gain)


def _by_weights_kernel(nx, dq, dk, dv, ot, dy, oq, ok, ov, oo):
    t = nx[...].T
    for g, o in ((dq, oq), (dk, ok), (dv, ov)):
        o[...] = _dot(t, g[...], 1, 0).astype(jnp.bfloat16)
    oo[...] = _dot(ot[...], dy[...], 1, 0).astype(jnp.bfloat16)


def by_weights(nx, grads, ot, dy, tile=BY_TILE):
    rows, d = nx.shape
    nq = ot.shape[0]
    whole = lambda t: pl.BlockSpec(t.shape, lambda j: (0, 0))
    columns = lambda n: pl.BlockSpec((n, tile), lambda j: (0, j))
    depth = sum(t.shape[1] for t in grads)
    return pl.pallas_call(
        _by_weights_kernel,
        grid=(d // tile,),
        in_specs=[columns(rows), *map(whole, grads), whole(ot), columns(rows)],
        out_specs=[pl.BlockSpec((tile, t.shape[1]), lambda j: (j, 0)) for t in grads] + [columns(nq)],
        out_shape=[jax.ShapeDtypeStruct((d, t.shape[1]), jnp.bfloat16) for t in grads] + [jax.ShapeDtypeStruct((nq, d), jnp.bfloat16)],
        compiler_params=_params(38),
        cost_estimate=_cost(2 * rows * d * (depth + nq), 2 * d * (2 * rows + depth + nq)),
        name="by_weights",
    )(nx, *grads, ot, dy)


ACROSS = [(0, 2), (1, 3), (2, 0), (3, 1)]
BESIDE = [(0, 1), (1, 0), (2, 3), (3, 2)]
CORNER = [(0, 3), (1, 2), (2, 1), (3, 0)]
CHUNKS = (2048, 3072)


def solution(mesh):
    def step(x, dy, gain, wq, wk, wv, wo):
        me = lax.axis_index("tp")
        own, d = x.shape
        rows = 4 * own
        half = HEAD // 2

        def send(t, way):
            return lax.ppermute(t, "tp", way)

        tie = lax.optimization_barrier

        table = []
        for i in range(4):
            role = [i ^ 1, (i + 2) % 4 ^ 1, i, (i + 2) % 4]
            n = own // PIECE
            table.append([role[2], role[0], role[3], role[1]] + [n * role[b] + p for p in range(n) for b in (3, 1)] + [role.index(b) for b in range(4)])
        pos = lax.dynamic_index_in_dim(jnp.array(table, jnp.int32), me, 0, keepdims=False)
        LOCAL, FAR, FAR_PIECES = 0, 2, 4
        ROLES = FAR_PIECES + 2 * (own // PIECE)

        xp = send(x, BESIDE)
        xa = send(x, ACROSS)
        ya = [send(dy[a : a + PIECE], ACROSS) for a in range(0, own, PIECE)]
        yp = send(dy, BESIDE)

        place = jnp.arange(rows)
        angle = place.astype(jnp.float32)[:, None] * THETA ** (-jnp.arange(half, dtype=jnp.float32) / half)
        cos, sin = jnp.cos(angle), jnp.sin(angle)
        cos, sin = jnp.concatenate([cos, cos], 1), jnp.concatenate([-sin, sin], 1)

        row_gain = gain[None]
        near = project(rows, pos, LOCAL, (2, 0), (x, xp), row_gain, cos, sin, wq, wk, wv, None)
        pos_1, near = tie((pos, near))
        back = back_out(rows, pos_1, LOCAL, own, (dy, yp), wo, None)
        xa, near, back = tie((xa, near, back))
        wide, back = tie((x, back))
        wide = wide.astype(jnp.float32)
        scale = jnp.broadcast_to(lax.rsqrt(jnp.mean(wide * wide, -1, keepdims=True) + 1e-6), (own, HEAD))
        pos_2, scale = tie((pos, scale))
        nx, q, k, v = project(rows, pos_2, FAR, (3, 1), (xa, send(xa, BESIDE)), row_gain, cos, sin, wq, wk, wv, near)
        pt, ot = attend(q, k, v)
        pt, ot, ya[0], back = tie((pt, ot, ya[0], back))
        back = back_out(rows, pos, FAR_PIECES, PIECE, (ya[0], send(ya[0], BESIDE)), wo, back)
        last, (dy_all, dat) = tie((ya[1], back))
        *grads, dy_all = attend_back(pos, FAR_PIECES + 2, ROLES, (last, send(last, BESIDE)), q, k, v, dat, wo, dy_all, ot, pt, cos, sin)

        weights = (wq, wk, wv)
        first, kept, sent = 0, [], []
        for c, width in enumerate(CHUNKS):
            stays, leaves = terms(c, grads, weights, first, width)
            stays, leaves, grads = tie((stays, leaves, grads))
            kept.append(stays)
            sent.append(send(leaves, ACROSS))
            first += width
        nx, leaves = tie((nx, leaves))
        *by_qkv, by_wo = by_weights(nx, grads, ot, dy_all)
        sent, by_wo = tie((sent, by_wo))
        wide_gain, n = gain.astype(jnp.float32)[None], len(CHUNKS)
        by_gain, cut = _by_rows(functools.partial(_sums_kernel, n=n), (*kept, *sent, x, scale), wide_gain,
                                [jax.ShapeDtypeStruct((1, d), jnp.float32), jax.ShapeDtypeStruct((own, HEAD), jnp.float32)])
        others = [send(by_gain, way) for way in (BESIDE, ACROSS, CORNER)]
        by_x, = _by_rows(functools.partial(_finish_kernel, n=n), (*kept, *sent, x, dy, scale, cut), wide_gain,
                         [jax.ShapeDtypeStruct((own, d), jnp.bfloat16)])
        by_gain = by_gain + others[0] + (others[1] + others[2])
        return (by_x, by_gain, *by_qkv, by_wo)

    tokens, columns = P(("dp", "tp"), None), P(None, "tp")

    return jax.shard_map(
        step,
        mesh=mesh,
        in_specs=(tokens, tokens, P(None), columns, columns, columns, P("tp", None)),
        out_specs=(tokens, P("dp", None), P("dp", "tp"), P("dp", "tp"), P("dp", "tp"), P(("dp", "tp"), None)),
        check_vma=False,
    )
```
